32 devices in a mesh: ep: 16 (over z, x, core), dp: 2 (over y).
Axes of the slice: x: 2, y: 2, z: 4, core: 2. Of those that a mesh axis runs over, the one named last changes fastest.
Arguments:
- tokens: bfloat16 [4096, 2048], P(('dp', 'ep')), parts along dimension 0, may hold values from -6 to 6
- expert_ids: int32 [4096, 8], P(('dp', 'ep')), parts along dimension 0, may hold values from 0 to 15, all different within a row; in each aligned block of 128 rows (0 to 127, 128 to 255, ...) at most 96 rows name the same one
- route_logits: float32 [4096, 8], P(('dp', 'ep')), parts along dimension 0, may hold values from -3 to 300
- w_gate: bfloat16 [16, 2048, 1024], P('ep'), may hold values from -0.125 to 0.125
- w_up: bfloat16 [16, 2048, 1024], P('ep'), may hold values from -0.125 to 0.125
- w_down: bfloat16 [16, 1024, 2048], P('ep'), may hold values from -0.1875 to 0.1875
Outputs:
- mixed_rows: bfloat16 [4096, 2048], P(('dp', 'ep')), parts along dimension 0
The draws below stay inside these ranges and needn't reach their ends.
There are 2 independent parts, one for each index of `dp`. The reference program is written for one: setup_inputs(seed, part) draws one part's arguments, and reference() takes and returns one part's arrays. A program takes and returns all parts, laid end to end along the dimension named above; an argument that names none is the same for every part. Nothing has to cross between parts.
Inputs may be any that keep to these rules, and one draw needn't show every extreme that they name: `expert_ids`: each row names 8 different experts; among the 128 rows of one device no expert is named more than 96 times, a bound that some block reaches.
All inputs are finite; a program needn't handle non-finite values.
Results may differ from the reference program's by a relative error of at most 0.0058.
Values may be sent and summed in bfloat16 or wider, within the bound.
A program may use at most 128 MiB of HBM per device.

```python
import math
import jax
import jax.numpy as jnp
import numpy as np
from jax import lax

D = 2048
FF = 1024
TOP = 8
TOK_DEV = 128
EXPERTS = 16
TOKENS = 2048
CAP = 96
N_EP = 16


def draw_route_logits(key, part):
    first_key = jax.random.fold_in(key, 11)
    values = jnp.clip(jax.random.normal(first_key, (TOKENS, TOP), jnp.float32) * 0.4, -0.75, 0.75)
    return values


def block_scale(key, extent, shards, smallest, top_value):
    loudness, own = 1.0, jax.random.fold_in(key, 6)
    for dim, shards_of in shards:
        steps = jnp.exp(jax.random.uniform(jax.random.fold_in(own, dim), (shards_of,), jnp.float32, smallest / len(shards), top_value / len(shards)))
        loudness = loudness * jnp.repeat(steps, extent[dim] // shards_of).reshape([-1 if axis == dim else 1 for axis in range(len(extent))])
    return loudness


def shared_out(stream_key, own, number, rows, number_of, top, bound, skew):
    ranking = jax.random.permutation(stream_key, number_of)
    packed, ordinary = shares(number_of, rows * top, bound, skew, True), shares(number_of, rows * top, bound, skew, False)
    places = jnp.arange(number_of)

    def named(sizes, turn):
        used = int((sizes > 0).sum())
        fixed = max(1, used // 4)
        moved = fixed + (places - fixed + turn * (used - fixed)) % max(1, number_of - fixed)
        return jnp.zeros((number_of,), jnp.int32).at[ranking[jnp.where(places < fixed, places, moved)]].set(jnp.asarray(sizes, jnp.int32))

    sizes = jnp.where(number % 4 == 0, named(packed, number // 4), named(ordinary, number - number // 4 - 1))
    mixed = jax.random.permutation(jax.random.fold_in(own, 3), number_of)
    source_of, sink = mixed[0:number_of // 2 * 2:2], mixed[1:number_of // 2 * 2:2]
    slack = jnp.minimum(sizes[source_of] - 1, bound - sizes[sink]) // 2
    slack = jnp.where((source_of == ranking[0]) | (sink == ranking[0]) | (sizes[sink] == 0), 0, jnp.maximum(slack, 0))
    moved = jax.random.randint(jax.random.fold_in(own, 4), (number_of // 2,), 0, 1 << 20) % (slack + 1)
    sizes = sizes.at[source_of].add(-moved).at[sink].add(moved)
    members = jnp.searchsorted(jnp.cumsum(sizes), jnp.arange(rows * top), side="right").astype(jnp.int32)
    grid = members.reshape(top, rows).T
    grid = grid[jax.random.permutation(jax.random.fold_in(own, 1), rows)]
    turn = jax.random.randint(jax.random.fold_in(own, 2), (rows, 1), 0, top)
    return jnp.take_along_axis(grid, (jnp.arange(top)[None, :] + turn) % top, axis=1)


def shares(count, total, bound, skew, full):
    loads = [(1 << 20) // math.isqrt(grade ** skew) + 1 for grade in range(1, count + 1)]
    largest = bound if full else min(bound, max(-(-total // count), total * loads[0] // sum(loads)))
    least = 1 if total - largest >= count - 1 else 0
    given, rest = [largest] + [least] * (count - 1), total - largest - least * (count - 1)
    while rest > 0:
        movable = [i for i in range(1, count) if given[i] < largest] or [i for i in range(1, count) if given[i] < bound]
        pool, left = sum([loads[i] for i in movable]), rest
        for i in movable:
            more = min(bound - given[i], max(1, left * loads[i] // pool), rest)
            given[i] = given[i] + more
            rest = rest - more
    return np.array(given)


def centred(own_key, extent, scale, bound, pieces=(), kind=jnp.bfloat16):
    values = jax.random.normal(own_key, extent, jnp.float32) * scale
    if len(pieces) > 0:
        values = block_scale(own_key, extent, pieces, -0.22, 0.18) * values
    return jnp.clip(values, min=-bound, max=bound).astype(kind)


def setup_inputs(seed: int = 0, part: int = 0) -> dict:
    key_list = jax.random.split(jax.random.key(seed), 7)
    part_keys = jax.random.split(jax.random.fold_in(key_list[6], part), 7)
    tokens = centred(part_keys[0], (TOKENS, D), 1.0, 6.0, ((0, 16),))
    expert_ids_keys = jax.random.split(jax.random.fold_in(part_keys[1], 1), TOKENS // TOK_DEV)
    expert_ids_turns = jax.random.permutation(jax.random.fold_in(part_keys[1], 3), TOKENS // TOK_DEV)
    expert_ids = jax.vmap(lambda own, number: shared_out(jax.random.fold_in(part_keys[1], 2), own, number, TOK_DEV, EXPERTS, TOP, CAP, 2))(expert_ids_keys, expert_ids_turns).reshape((TOKENS, TOP))
    route_logits = draw_route_logits(jax.random.fold_in(jax.random.fold_in(key_list[6], part), 71), part)
    w_gate = centred(key_list[3], (EXPERTS, D, FF), D ** -0.5, 0.125, ((0, 16),))
    w_up = centred(key_list[4], (EXPERTS, D, FF), D ** -0.5, 0.125, ((0, 16),))
    w_down = centred(key_list[5], (EXPERTS, FF, D), FF ** -0.5, 0.1875, ((0, 16),))
    return {"tokens": tokens, "expert_ids": expert_ids, "route_logits": route_logits, "w_gate": w_gate, "w_up": w_up, "w_down": w_down}


def expert_ffn(rows, gate_weight, up_weight, down_weight):
    gate = jnp.dot(rows, gate_weight, preferred_element_type=jnp.float32)
    up_part = jnp.dot(rows, up_weight, preferred_element_type=jnp.float32)
    hidden = (jax.nn.silu(gate) * up_part).astype(jnp.bfloat16)
    return jnp.dot(hidden, down_weight, preferred_element_type=jnp.float32).astype(jnp.bfloat16)


def reference(tokens, expert_ids, route_logits, w_gate, w_up, w_down):
    token_count, model_width = tokens.shape
    picks = expert_ids.shape[1]
    gates = jax.nn.softmax(route_logits.astype(jnp.float32), axis=-1)
    flat_ids = expert_ids.reshape(-1)
    flat_gates = gates.reshape(-1)
    flat_token = (jnp.arange(token_count * picks, dtype=jnp.int32) // picks).astype(jnp.int32)
    buffer = N_EP * CAP
    padded = jnp.concatenate([tokens, jnp.zeros((1, model_width), tokens.dtype)], 0)

    def expert_pass(mixed, inputs):
        gate_weight, up_weight, down_weight, expert = inputs
        chosen = flat_ids == expert
        place = (jnp.cumsum(chosen.astype(jnp.int32)) - 1).astype(jnp.int32)
        target = jnp.where(chosen, place, buffer).astype(jnp.int32)
        rows_token = jnp.full((buffer,), token_count, jnp.int32).at[target].set(flat_token, mode="drop")
        rows_gate = jnp.zeros((buffer,), jnp.float32).at[target].set(flat_gates, mode="drop")
        answer = expert_ffn(padded[rows_token], gate_weight, up_weight, down_weight)
        mixed = mixed.at[rows_token].add(rows_gate[:, None] * answer.astype(jnp.float32), mode="drop")
        return mixed, None

    start = jnp.zeros((token_count, model_width), jnp.float32)
    mixed, _ = lax.scan(expert_pass, start, (w_gate, w_up, w_down, jnp.arange(EXPERTS, dtype=jnp.int32)))
    return mixed.astype(jnp.bfloat16)
```

```python
import functools

import jax
import jax.numpy as jnp
from jax import lax
from jax.experimental import pallas as pl
from jax.experimental.pallas import tpu as pltpu
from jax.sharding import PartitionSpec as P

VMEM_BYTES = 63 * 1024 * 1024

KINDS = (1, 0, 0, 1, 0, 1, 0, 0)
END_BATCHES = (
    5, 2, 0, 3, 0, 0, 0, 1, 3, 2, 7, 7, 4, 6, 2, 3,
    7, 5, 3, 6, 1, 0, 1, 1, 6, 7, 6, 7, 6, 6, 2, 5,
    4, 3, 1, 0, 0, 1, 3, 3, 0, 4, 2, 4, 4, 4, 1, 5,
    5, 3, 2, 7, 7, 6, 5, 4, 1, 4, 5, 5, 7, 6, 2, 2,
)
MID_BATCHES = (
    6, 6, 0, 0, 0, 1, 4, 4, 0, 2, 5, 2, 1, 2, 7, 0,
    3, 7, 3, 1, 3, 0, 6, 6, 6, 4, 5, 5, 1, 3, 4, 6,
    7, 1, 6, 1, 4, 2, 5, 3, 7, 5, 2, 3, 3, 2, 0, 5,
    7, 4, 5, 4, 1, 4, 2, 2, 7, 6, 7, 5, 1, 3, 7, 0,
)
END_ORDER = (
    400, 200, 0, 600, 10, 401, 700, 201, 500, 1, 410, 601, 100, 701, 20, 300,
    420, 501, 411, 220, 101, 11, 210, 301, 430, 30, 421, 610, 221, 230, 21, 211,
    1000, 530, 431, 1010, 1020, 730, 611, 1030, 31, 231, 1040, 1050, 130, 1100, 1110, 330,
    1120, 2030, 2221, 2021, 731, 2411, 510, 1130, 1140, 630, 131, 2020, 1150, 2010, 1200, 110,
    1210, 1220, 511, 2530, 2421, 1230, 520, 2231, 2031, 1240, 631, 2410, 1250, 120, 1300, 111,
    710, 2220, 1310, 1320, 521, 2101, 2330, 1330, 2230, 2731, 531, 1340, 1350, 310, 121, 2420,
    1400, 711, 2510, 1410, 331, 2131, 2431, 1420, 2011, 1430, 720, 2730, 1440, 1450, 620, 1500,
    311, 2130, 2401, 1510, 320, 2521, 1520, 2430, 2631, 1530, 721, 2601, 321, 1540, 2511, 1550,
    621, 2701, 2520, 2531, 2711, 1600, 2201, 1610, 2331, 1620, 2630, 1630, 1640, 1650, 2001, 2710,
    1700, 1710, 2321, 2121, 2320, 2721, 1720, 1730, 2310, 2621, 1740, 2000, 2211, 1750, 2400, 2120,
    2311, 2111, 2720, 2611, 2620, 2501, 2210, 2301, 2110, 2600, 2610, 2500, 2200, 2300, 2700, 2100,
)
MID_ORDER = (
    0, 400, 200, 600, 430, 10, 401, 410, 30, 201, 230, 601, 210, 1, 431, 420,
    411, 530, 730, 20, 231, 220, 31, 211, 11, 130, 421, 520, 330, 731, 630, 720,
    221, 21, 531, 131, 120, 331, 631, 320, 721, 500, 121, 620, 100, 1000, 501, 1010,
    621, 510, 1020, 1030, 101, 110, 1040, 1050, 700, 1100, 1110, 511, 1120, 2221, 111, 2731,
    521, 2011, 2020, 1130, 1140, 701, 300, 1150, 2131, 1200, 321, 2010, 1210, 710, 1220, 2021,
    1230, 610, 1240, 2401, 1250, 301, 1300, 310, 2411, 1310, 711, 2320, 1320, 2121, 1330, 611,
    2111, 1340, 311, 1350, 2631, 1400, 1410, 2421, 1420, 2520, 2721, 2220, 1430, 1440, 2431, 1450,
    2120, 1500, 2101, 1510, 2031, 2030, 2511, 2611, 1520, 2420, 1530, 2530, 2720, 2621, 1540, 2330,
    2211, 1550, 2510, 2601, 1600, 2521, 1610, 2711, 2430, 1620, 2321, 2501, 1630, 2620, 1640, 2210,
    1650, 1700, 2531, 1710, 2311, 2231, 2331, 2410, 2001, 1720, 1730, 2310, 2630, 2701, 1740, 1750,
    2110, 2230, 2301, 2000, 2500, 2730, 2201, 2130, 2400, 2710, 2610, 2300, 2200, 2700, 2100, 2600,
)
ORDERS = (END_ORDER, MID_ORDER)


def expert_ffn(rows, gate_weight, up_weight, down_weight):
    gate = jnp.dot(rows, gate_weight, preferred_element_type=jnp.float32)
    up_part = jnp.dot(rows, up_weight, preferred_element_type=jnp.float32)
    hidden = (jax.nn.silu(gate) * up_part).astype(jnp.bfloat16)
    return jnp.dot(hidden, down_weight, preferred_element_type=jnp.float32).astype(jnp.bfloat16)


def blockwise(rows, live_rows, weights):
    turns = (live_rows + 127) // 128

    def step(block_index, result):
        first_row = block_index * 128
        block_rows = lax.dynamic_slice_in_dim(rows, first_row, 128, 0)
        answer = expert_ffn(block_rows, weights[0], weights[1], weights[2])
        return lax.dynamic_update_slice_in_dim(result, answer, first_row, 0)

    return lax.fori_loop(jnp.int32(0), turns, step, jnp.zeros(rows.shape, jnp.bfloat16))


def per_device(tokens, expert_ids, route_logits, w_gate, w_up, w_down):
    tok_rows, model_width = tokens.shape
    picks = expert_ids.shape[1]
    experts = lax.axis_size("ep")
    capacity = min(tok_rows, 3 * tok_rows * picks // (2 * experts))
    row_quota = tok_rows * picks
    received = experts * capacity
    spill_count = (max(received - row_quota, 128) + 127) // 128 * 128
    length = row_quota + spill_count
    flat_ids = expert_ids.reshape(-1)
    one_hot = (flat_ids[:, None] == jnp.arange(experts, dtype=jnp.int32)[None, :]).astype(jnp.int32)
    earlier = jnp.cumsum(one_hot, axis=0) - one_hot
    slot_rank = jnp.sum(earlier * one_hot, axis=1)
    counts = jnp.sum(one_hot, axis=0)
    slot_place = flat_ids * capacity + slot_rank
    source_row = jnp.arange(row_quota, dtype=jnp.int32) // picks
    slot_token = jnp.full((received,), tok_rows, jnp.int32).at[slot_place].set(source_row)
    padded_tokens = jnp.concatenate([tokens, jnp.zeros((1, model_width), tokens.dtype)], 0)
    outgoing = padded_tokens[slot_token].reshape(experts, capacity, model_width)
    all_counts = lax.all_gather(counts, "ep", axis=0, tiled=True).reshape(experts, experts)
    own_index = lax.axis_index("ep")
    from_sources = lax.dynamic_index_in_dim(all_counts, own_index, 1, keepdims=False)
    incoming = lax.all_to_all(outgoing, "ep", split_axis=0, concat_axis=0, tiled=True)
    offsets = jnp.cumsum(from_sources) - from_sources
    live_rows = jnp.sum(from_sources)
    slot_numbers = jnp.arange(capacity, dtype=jnp.int32)
    live_slot = slot_numbers[None, :] < from_sources[:, None]
    position = jnp.where(live_slot, offsets[:, None] + slot_numbers[None, :], length).reshape(-1)
    gather_order = (
        jnp.full((length,), received, jnp.int32)
        .at[position]
        .set(jnp.arange(received, dtype=jnp.int32), mode="drop")
    )
    flat_incoming = jnp.concatenate(
        [incoming.reshape(received, model_width), jnp.zeros((1, model_width), jnp.bfloat16)], 0
    )
    packed = flat_incoming[gather_order]
    own_weights = (w_gate[0], w_up[0], w_down[0])
    results = blockwise(packed, live_rows, own_weights)
    results_ext = jnp.concatenate([results, jnp.zeros((1, model_width), jnp.bfloat16)], 0)
    outgoing_back = results_ext[position].reshape(experts, capacity, model_width)
    answers = lax.all_to_all(outgoing_back, "ep", split_axis=0, concat_axis=0, tiled=True)
    mix_weights = jax.nn.softmax(route_logits, axis=-1)
    picked = answers.reshape(received, model_width)[slot_place].reshape(
        tok_rows, picks, model_width
    )
    mixed_rows = jnp.zeros((tok_rows, model_width), jnp.float32)
    for column in range(picks):
        mixed_rows = mixed_rows + mix_weights[:, column : column + 1] * picked[:, column].astype(
            jnp.float32
        )
    return mixed_rows.astype(jnp.bfloat16)


def remote(src, dst, send_sem, recv_sem, target):
    return pltpu.make_async_remote_copy(
        src_ref=src,
        dst_ref=dst,
        send_sem=send_sem,
        recv_sem=recv_sem,
        device_id={"ep": target},
        device_id_type=pl.DeviceIdType.MESH,
    )


PIECES = len(KINDS)
CELLS = [(p, d, c) for p in range(PIECES) for d in range(4) for c in range(2)]
PARTS = 6


def slots_of(batches):
    filled, table = [0] * PIECES, {}
    for cell, batch in zip(CELLS, batches):
        table[cell] = (batch, filled[batch])
        filled[batch] += 1
    return table


SLOT = (slots_of(END_BATCHES), slots_of(MID_BATCHES))


def at(cell):
    return (cell[0] * 4 + cell[1]) * 2 + cell[2]


def place_of(cell):
    return cell[1] * 2 + cell[2]


def moves(role, cell):
    p, d, c = cell
    first_z = KINDS[p] == 0
    out = []
    if d == 0 and (c == 0 or not first_z):
        if role == 0:
            out.append(("in", 1, (p, 3, c)))
        else:
            out.append(("out", 0, (p, 1, c)))
            out.append(("in", 1, (p, 1, c)))
    elif d > 0 and (c == 0 or not first_z) and role == 1:
        if d == 3:
            out.append(("in", 1, (p, 2, c)))
        else:
            out.append(("out", 0, (p, d + 1, c)))
    if c == 0 and (first_z or d == 0):
        across = ("x", role, (p, d, 1))
        out = out + [across] if first_z else [across] + out
    return out


def fused_kernel(
    n,
    tok_ref,
    ids_ref,
    logits_ref,
    wg_hbm,
    wu_hbm,
    wd_hbm,
    out_ref,
    xs,
    wg,
    wu,
    wd,
    ps,
    sib,
    put,
    got_x,
    got_in,
    got_out,
    hid,
    gates,
    gate_tok,
    gate_col,
    load_sem,
    tok_sem,
    ag_send,
    ag_recv,
    twin_send,
    twin_recv,
    gate_send,
    gate_recv,
    gate_pass,
    sib_send,
    sib_recv,
    rs_send,
    x_recv,
    in_recv,
    out_recv,
):
    tok_rows, width = tok_ref.shape
    rows = tok_rows // PIECES
    ff = wg.shape[1]
    me = lax.axis_index("ep")
    core, chip = me % 2, me // 2
    other = 1 - core
    x, z = chip % 2, chip // 2
    depth = n // 4
    inward = jnp.where(z < depth // 2, 1, -1)
    at_end = jnp.logical_or(z == 0, z == depth - 1)
    at_mid = jnp.logical_not(at_end)
    peers = {
        "in": ((z + inward) * 2 + x) * 2 + core,
        "out": ((z - inward) * 2 + x) * 2 + core,
        "x": (z * 2 + 1 - x) * 2 + core,
        "twin": chip * 2 + other,
    }

    def by_role(end_part, mid_part):
        if end_part is not None:
            pl.when(at_end)(end_part)
        if mid_part is not None:
            pl.when(at_mid)(mid_part)

    barrier = pltpu.get_barrier_semaphore()

    def greet(friend):
        pl.semaphore_signal(
            barrier,
            inc=1,
            device_id={"ep": peers[friend]},
            device_id_type=pl.DeviceIdType.MESH,
        )

    greet("twin")
    greet("x")
    greet("in")
    by_role(None, lambda: greet("out"))

    def chunk(role, cell, whose):
        batch, place = SLOT[role][cell]
        return xs.at[(batch * PIECES + place) * 2 + whose]

    def own_load(role, p):
        return pltpu.make_async_copy(
            tok_ref.at[pl.ds(p * rows, rows)], chunk(role, (p, 0, 0), core), tok_sem.at[p]
        )

    def load_all(role):
        for code in ORDERS[role]:
            if code // 1000 == 0 and code % 100 == 0:
                own_load(role, code // 100).start()

    by_role(lambda: load_all(0), lambda: load_all(1))
    weight_loads = [
        pltpu.make_async_copy(wg_hbm.at[0], wg, load_sem.at[0]),
        pltpu.make_async_copy(wu_hbm.at[0], wu, load_sem.at[1]),
        pltpu.make_async_copy(wd_hbm.at[0], wd, load_sem.at[2]),
    ]
    for load in weight_loads:
        load.start()

    logits = logits_ref[...]
    powers = jnp.exp(logits - jnp.max(logits, axis=0, keepdims=True))
    shares = powers / jnp.sum(powers, axis=0, keepdims=True)
    ids = ids_ref[...]
    for expert in range(n):
        gates[core, expert] = jnp.sum(
            jnp.where(ids == expert, shares, 0.0), axis=0, keepdims=True
        )

    by_role(lambda: pl.semaphore_wait(barrier, 3), lambda: pl.semaphore_wait(barrier, 4))

    def ag_copy(role, cell, link, to_role, to_cell):
        return remote(
            chunk(role, cell, core),
            chunk(to_role, to_cell, core),
            ag_send.at[0],
            ag_recv.at[at(to_cell)],
            peers[link],
        )

    def pass_copy(role, cell, whose):
        batch, place = SLOT[role][cell]
        ref = chunk(role, cell, whose)
        return remote(ref, ref, twin_send.at[0], twin_recv.at[batch], peers["twin"])

    def gate_copy(cell, link, to_cell):
        return remote(
            gates.at[place_of(cell) * 2 + core],
            gates.at[place_of(to_cell) * 2 + core],
            gate_send.at[0],
            gate_recv.at[place_of(to_cell)],
            peers[link],
        )

    def gate_twin(cell, whose):
        place = place_of(cell)
        ref = gates.at[place * 2 + whose]
        return remote(ref, ref, gate_send.at[1], gate_pass.at[place], peers["twin"])

    def receive(role, cell):
        p, d, c = cell
        lead = p == 0
        if (d, c) == (0, 0):
            own_load(role, p).wait()
        else:
            if lead:
                gate_copy(cell, "x", cell).wait_recv()
            ag_copy(role, cell, "x", role, cell).wait_recv()
        for link, to_role, to_cell in moves(role, cell):
            if lead:
                gate_copy(cell, link, to_cell).start()
            ag_copy(role, cell, link, to_role, to_cell).start()
        if lead:
            gate_twin(cell, core).start()
        pass_copy(role, cell, core).start()

    def sib_copy(batch, half, whose):
        cols = pl.ds(half * (width // 2), width // 2)
        return remote(
            ps.at[batch, :, whose, :, cols],
            sib.at[batch, :, :, cols],
            sib_send.at[0],
            sib_recv.at[batch],
            peers["twin"],
        )

    sib_seen = (set(), set())
    put_used = [0, 0]

    def send_back(role, cell):
        p, d, c = cell
        first_z = KINDS[p] == 0
        batch, place = SLOT[role][cell]
        if batch not in sib_seen[role]:
            sib_seen[role].add(batch)
            ref = sib.at[batch]
            remote(ref, ref, sib_send.at[0], sib_recv.at[batch], peers["twin"]).wait_recv()
        total = ps[batch, place, core].astype(jnp.float32) + sib[batch, place].astype(jnp.float32)
        inbox = []
        if c == 0 and (first_z or d == 0):
            inbox.append((got_x, x_recv, p * 4 + d))
        if c == 0 or not first_z:
            if d == 0 or (d == 3 and role == 1):
                inbox.append((got_in, in_recv, (p * 2 + d // 3) * 2 + c))
            if role == 1 and d < 3:
                inbox.append((got_out, out_recv, (p * 3 + d) * 2 + c))
        for buffer, sem, index in inbox:
            ref = buffer.at[index]
            remote(ref, ref, rs_send.at[0], sem.at[index], peers["x"]).wait_recv()
            total = total + buffer[index].astype(jnp.float32)
        total = total.astype(jnp.bfloat16)
        if c == 1 and (first_z or d == 0):
            link, buffer, sem, index = "x", got_x, x_recv, p * 4 + d
        elif d == 0:
            out_ref[pl.ds(p * rows, rows), :] = total
            return
        elif role == 0:
            link, buffer, sem, index = "in", got_out, out_recv, (p * 3 + d - 1) * 2 + c
        elif d == 3:
            link, buffer, sem, index = "out", got_in, in_recv, p * 4 + c
        else:
            link, buffer, sem, index = "in", got_in, in_recv, (p * 2 + d - 1) * 2 + c
        slot = put_used[role]
        put_used[role] += 1
        put[slot] = total
        remote(put.at[slot], buffer.at[index], rs_send.at[0], sem.at[index], peers[link]).start()

    ff_tile = ff // 4
    out_tile = width // 4

    def hidden_part(batch, first, last):
        def body(j, carry):
            rows_in = xs[pl.ds(batch * 2 * PIECES, 2 * PIECES)].reshape(2 * tok_rows, width)
            cols = pl.ds(pl.multiple_of(j * ff_tile, ff_tile), ff_tile)
            gate = jnp.dot(rows_in, wg[:, cols], preferred_element_type=jnp.float32)
            up = jnp.dot(rows_in, wu[:, cols], preferred_element_type=jnp.float32)
            hid[:, cols] = (gate / (1.0 + jnp.exp(-gate)) * up).astype(jnp.bfloat16)
            return carry

        lax.fori_loop(first, last, body, 0)

    def answer_part(batch, first, last):
        def body(j, carry):
            cols = pl.ds(pl.multiple_of(j * out_tile, out_tile), out_tile)
            answer = jnp.dot(hid[...], wd[:, cols], preferred_element_type=jnp.float32)
            scale = jnp.concatenate([gate_col[...]] * (out_tile // 128), axis=1)
            ps[batch, :, :, :, cols] = (
                (answer * scale).astype(jnp.bfloat16).reshape(PIECES, 2, rows, out_tile)
            )
            return carry

        lax.fori_loop(first, last, body, 0)

    gates_seen = (set(), set())

    def gate_fill(role, batch):
        for cell in CELLS:
            if SLOT[role][cell][0] != batch:
                continue
            p, d, c = cell
            source = place_of(cell)
            if source not in gates_seen[role]:
                gates_seen[role].add(source)
                gate_twin((0, d, c), other).wait_recv()
                for whose in range(2):
                    row = gates[source * 2 + whose, me]
                    gate_tok[source * 2 + whose] = jnp.broadcast_to(row, (128, tok_rows)).T
            for whose in range(2):
                first = (SLOT[role][cell][1] * 2 + whose) * rows
                gate_col[pl.ds(first, rows), :] = gate_tok[source * 2 + whose, pl.ds(p * rows, rows), :]

    def compute(batch, first, last):
        if first == 0:
            ref = xs.at[pl.ds(0, PIECES)]
            remote(ref, ref, twin_send.at[0], twin_recv.at[batch], peers["twin"]).wait_recv()
            if batch == 0:
                weight_loads[0].wait()
                weight_loads[1].wait()
        if first < 4:
            hidden_part(batch, first, min(last, 4))
        if first <= 4 < last:
            by_role(lambda: gate_fill(0, batch), lambda: gate_fill(1, batch))
            if batch == 0:
                weight_loads[2].wait()
        for part in range(max(first, 4), last):
            answer_part(batch, (part - 4) * 2, (part - 3) * 2)
            sib_copy(batch, part - 4, other).start()

    def events(role, codes):
        if not codes:
            return None

        def run():
            for code in codes:
                cell = (code // 100 % 10, code // 10 % 10, code % 10)
                if code < 1000:
                    receive(role, cell)
                else:
                    send_back(role, cell)

        return run

    plans = []
    for order in ORDERS:
        plan, now = [], []
        for code in order:
            if code // 1000 == 1:
                plan.append((now, code))
                now = []
            else:
                now.append(code)
        plan.append((now, None))
        plans.append(plan)

    waiting = None
    for (end_codes, code), (mid_codes, mid_code) in zip(*plans):
        assert code == mid_code
        batch, part = (None, None) if code is None else (code // 100 % 10, code // 10 % 10)
        if waiting is not None and (end_codes or mid_codes or batch != waiting[0]):
            compute(*waiting)
            waiting = None
        by_role(events(0, end_codes), events(1, mid_codes))
        if code is not None:
            waiting = (batch, part, part + 1) if waiting is None else (batch, waiting[1], part + 1)

    def finish(role):
        sent = sum(len(moves(role, cell)) for cell in CELLS)
        ref = xs.at[pl.ds(0, sent)]
        remote(ref, ref, ag_send.at[0], ag_recv.at[0], peers["x"]).wait_send()
        sent = sum(len(moves(role, cell)) for cell in CELLS if cell[0] == 0)
        ref = gates.at[pl.ds(0, sent)]
        remote(ref, ref, gate_send.at[0], gate_recv.at[0], peers["x"]).wait_send()

    by_role(lambda: finish(0), lambda: finish(1))
    ref = xs.at[pl.ds(0, len(CELLS))]
    remote(ref, ref, twin_send.at[0], twin_recv.at[0], peers["twin"]).wait_send()
    ref = gates.at[pl.ds(0, 8)]
    remote(ref, ref, gate_send.at[1], gate_pass.at[0], peers["twin"]).wait_send()
    remote(sib, sib, sib_send.at[0], sib_recv.at[0], peers["twin"]).wait_send()
    assert put_used == [put.shape[0]] * 2
    remote(put, put, rs_send.at[0], x_recv.at[0], peers["x"]).wait_send()


def fused_scratch(n, tok_rows, width, ff):
    bf16, f32 = jnp.bfloat16, jnp.float32
    rows = tok_rows // PIECES
    chunk = (rows, width)
    buffers = [
        ((PIECES * 16,) + chunk, bf16),
        ((width, ff), bf16),
        ((width, ff), bf16),
        ((ff, width), bf16),
        ((PIECES, 8, 2) + chunk, bf16),
        ((PIECES, 8) + chunk, bf16),
        ((PIECES * 7,) + chunk, bf16),
        ((PIECES * 4,) + chunk, bf16),
        ((PIECES * 4,) + chunk, bf16),
        ((PIECES * 6,) + chunk, bf16),
        ((2 * tok_rows, ff), bf16),
        ((16, n, 1, tok_rows), f32),
        ((16, tok_rows, 128), f32),
        ((2 * tok_rows, 128), f32),
    ]
    sems = [3, PIECES, 1, PIECES * 8, 1, PIECES, 2, 8, 8, 1, PIECES, 1]
    sems += [PIECES * 4, PIECES * 4, PIECES * 6]
    size = 0
    for shape, kind in buffers:
        count = jnp.dtype(kind).itemsize
        for extent in shape:
            count = count * extent
        size = size + count
    scratch = [pltpu.VMEM(shape, kind) for shape, kind in buffers]
    return scratch + [pltpu.SemaphoreType.DMA((count,)) for count in sems], size


def fused_device(tokens, expert_ids, route_logits, w_gate, w_up, w_down):
    n = lax.axis_size("ep")
    tok_rows, width = tokens.shape
    ff = w_gate.shape[2]
    scratch, size = fused_scratch(n, tok_rows, width, ff)
    anywhere, vmem = pl.BlockSpec(memory_space=pl.ANY), pl.BlockSpec(memory_space=pltpu.VMEM)
    return pl.pallas_call(
        functools.partial(fused_kernel, n),
        out_shape=jax.ShapeDtypeStruct((tok_rows, width), jnp.bfloat16),
        in_specs=[anywhere, vmem, vmem, anywhere, anywhere, anywhere],
        out_specs=vmem,
        scratch_shapes=scratch,
        compiler_params=pltpu.CompilerParams(
            collective_id=0, has_side_effects=True, vmem_limit_bytes=VMEM_BYTES
        ),
    )(tokens, expert_ids.T, route_logits.T, w_gate, w_up, w_down)


def layer(tokens, expert_ids, route_logits, w_gate, w_up, w_down):
    n = lax.axis_size("ep")
    tok_rows, width = tokens.shape
    ff = w_gate.shape[2]
    size = fused_scratch(n, tok_rows, width, ff)[1]
    fits = size + 8 * tok_rows * width < VMEM_BYTES and width % 512 == 0 and ff % 512 == 0
    if fits and n == 16 and tok_rows == 16 * PIECES:
        return fused_device(tokens, expert_ids, route_logits, w_gate, w_up, w_down)
    return per_device(tokens, expert_ids, route_logits, w_gate, w_up, w_down)


def solution(mesh):
    in_specs = (
        P(("dp", "ep"), None),
        P(("dp", "ep"), None),
        P(("dp", "ep"), None),
        P("ep", None, None),
        P("ep", None, None),
        P("ep", None, None),
    )
    out_specs = P(("dp", "ep"), None)
    return jax.shard_map(
        layer, mesh=mesh, in_specs=in_specs, out_specs=out_specs, check_vma=False
    )
```

```python
import functools

import jax
import jax.numpy as jnp
from jax import lax
from jax.experimental import pallas as pl
from jax.experimental.pallas import tpu as pltpu
from jax.sharding import PartitionSpec as P

VMEM_BYTES = 63 * 1024 * 1024

KINDS = (1, 0, 1, 0, 0, 1, 0, 0)
END_BATCHES = (
    7, 7, 1, 0, 0, 1, 1, 2, 3, 4, 6, 6, 6, 6, 5, 5,
    7, 5, 7, 7, 6, 6, 3, 3, 2, 5, 2, 7, 5, 6, 4, 4,
    3, 2, 0, 0, 0, 1, 2, 3, 5, 4, 4, 5, 5, 6, 2, 4,
    7, 4, 0, 1, 3, 4, 2, 3, 3, 7, 1, 0, 0, 1, 1, 2,
)
MID_BATCHES = (
    4, 2, 0, 2, 3, 3, 2, 2, 7, 4, 6, 6, 5, 4, 5, 2,
    7, 7, 6, 6, 3, 3, 7, 1, 0, 2, 6, 6, 3, 4, 4, 4,
    7, 6, 5, 3, 0, 2, 0, 5, 7, 7, 5, 5, 1, 3, 5, 1,
    1, 0, 1, 7, 1, 4, 5, 1, 6, 4, 0, 0, 0, 2, 1, 3,
)
END_ORDER = (
    700, 0, 600, 400, 701, 710, 10, 1, 500, 601, 410, 401, 610, 711, 720, 20,
    501, 200, 411, 420, 11, 611, 300, 1000, 30, 721, 100, 1010, 1020, 730, 201, 1030,
    421, 1040, 310, 1050, 21, 301, 31, 101, 2711, 2411, 2020, 2011, 1100, 731, 1110, 630,
    1120, 311, 1130, 430, 1140, 530, 1150, 620, 2410, 1200, 2611, 2710, 2721, 631, 2030, 230,
    1210, 1220, 330, 2021, 431, 1230, 621, 1240, 2421, 2010, 231, 1250, 2610, 130, 531, 1300,
    2720, 2731, 1310, 2530, 2401, 510, 331, 1320, 1330, 2420, 110, 1340, 1350, 320, 2031, 131,
    1400, 2730, 520, 1410, 2631, 210, 1420, 2431, 2231, 1430, 111, 1440, 120, 2230, 511, 1450,
    321, 211, 2630, 1500, 2531, 2621, 2331, 220, 1510, 2430, 1520, 2101, 121, 521, 2510, 1530,
    2601, 221, 1540, 1550, 2620, 1600, 1610, 2330, 2131, 2520, 2301, 1620, 1630, 2511, 1640, 1650,
    2201, 1700, 2130, 1710, 2521, 2321, 2121, 1720, 2221, 1730, 2111, 2220, 1740, 1750, 2501, 2320,
    2400, 2701, 2211, 2311, 2120, 2600, 2001, 2110, 2300, 2500, 2210, 2700, 2200, 2310, 2100, 2000,
)
MID_ORDER = (
    700, 0, 400, 600, 701, 710, 30, 10, 730, 401, 410, 601, 1, 430, 711, 20,
    31, 731, 720, 630, 411, 300, 431, 11, 530, 721, 21, 531, 631, 620, 230, 301,
    420, 330, 1000, 520, 130, 1010, 610, 621, 1020, 231, 1030, 421, 220, 1040, 1050, 320,
    331, 1100, 131, 1110, 120, 1120, 2711, 221, 611, 2010, 1130, 2601, 1140, 321, 521, 1150,
    1200, 121, 500, 1210, 1220, 2631, 100, 1230, 1240, 310, 1250, 510, 1300, 1310, 200, 1320,
    2421, 2011, 1330, 110, 101, 1340, 501, 1350, 311, 2301, 1400, 201, 2710, 2131, 1410, 210,
    1420, 2520, 2731, 1430, 111, 2020, 511, 2411, 1440, 1450, 211, 2021, 2721, 1500, 1510, 2701,
    1520, 2221, 2331, 1530, 2220, 2030, 1540, 2621, 1550, 2720, 2031, 2321, 1600, 2521, 2231, 1610,
    2530, 2410, 2431, 1620, 2420, 2101, 1630, 2730, 2620, 2121, 1640, 1650, 2531, 2001, 1700, 2320,
    1710, 2311, 2700, 2510, 1720, 2430, 2401, 1730, 2630, 2111, 1740, 2120, 1750, 2330, 2000, 2511,
    2230, 2611, 2211, 2400, 2130, 2210, 2501, 2310, 2610, 2201, 2110, 2500, 2600, 2200, 2100, 2300,
)
ORDERS = (END_ORDER, MID_ORDER)


def expert_ffn(rows, gate_weight, up_weight, down_weight):
    gate = jnp.dot(rows, gate_weight, preferred_element_type=jnp.float32)
    up_part = jnp.dot(rows, up_weight, preferred_element_type=jnp.float32)
    hidden = (jax.nn.silu(gate) * up_part).astype(jnp.bfloat16)
    return jnp.dot(hidden, down_weight, preferred_element_type=jnp.float32).astype(jnp.bfloat16)


def blockwise(rows, live_rows, weights):
    turns = (live_rows + 127) // 128

    def step(block_index, result):
        first_row = block_index * 128
        block_rows = lax.dynamic_slice_in_dim(rows, first_row, 128, 0)
        answer = expert_ffn(block_rows, weights[0], weights[1], weights[2])
        return lax.dynamic_update_slice_in_dim(result, answer, first_row, 0)

    return lax.fori_loop(jnp.int32(0), turns, step, jnp.zeros(rows.shape, jnp.bfloat16))


def per_device(tokens, expert_ids, route_logits, w_gate, w_up, w_down):
    tok_rows, model_width = tokens.shape
    picks = expert_ids.shape[1]
    experts = lax.axis_size("ep")
    capacity = min(tok_rows, 3 * tok_rows * picks // (2 * experts))
    row_quota = tok_rows * picks
    received = experts * capacity
    spill_count = (max(received - row_quota, 128) + 127) // 128 * 128
    length = row_quota + spill_count
    flat_ids = expert_ids.reshape(-1)
    one_hot = (flat_ids[:, None] == jnp.arange(experts, dtype=jnp.int32)[None, :]).astype(jnp.int32)
    earlier = jnp.cumsum(one_hot, axis=0) - one_hot
    slot_rank = jnp.sum(earlier * one_hot, axis=1)
    counts = jnp.sum(one_hot, axis=0)
    slot_place = flat_ids * capacity + slot_rank
    source_row = jnp.arange(row_quota, dtype=jnp.int32) // picks
    slot_token = jnp.full((received,), tok_rows, jnp.int32).at[slot_place].set(source_row)
    padded_tokens = jnp.concatenate([tokens, jnp.zeros((1, model_width), tokens.dtype)], 0)
    outgoing = padded_tokens[slot_token].reshape(experts, capacity, model_width)
    all_counts = lax.all_gather(counts, "ep", axis=0, tiled=True).reshape(experts, experts)
    own_index = lax.axis_index("ep")
    from_sources = lax.dynamic_index_in_dim(all_counts, own_index, 1, keepdims=False)
    incoming = lax.all_to_all(outgoing, "ep", split_axis=0, concat_axis=0, tiled=True)
    offsets = jnp.cumsum(from_sources) - from_sources
    live_rows = jnp.sum(from_sources)
    slot_numbers = jnp.arange(capacity, dtype=jnp.int32)
    live_slot = slot_numbers[None, :] < from_sources[:, None]
    position = jnp.where(live_slot, offsets[:, None] + slot_numbers[None, :], length).reshape(-1)
    gather_order = (
        jnp.full((length,), received, jnp.int32)
        .at[position]
        .set(jnp.arange(received, dtype=jnp.int32), mode="drop")
    )
    flat_incoming = jnp.concatenate(
        [incoming.reshape(received, model_width), jnp.zeros((1, model_width), jnp.bfloat16)], 0
    )
    packed = flat_incoming[gather_order]
    own_weights = (w_gate[0], w_up[0], w_down[0])
    results = blockwise(packed, live_rows, own_weights)
    results_ext = jnp.concatenate([results, jnp.zeros((1, model_width), jnp.bfloat16)], 0)
    outgoing_back = results_ext[position].reshape(experts, capacity, model_width)
    answers = lax.all_to_all(outgoing_back, "ep", split_axis=0, concat_axis=0, tiled=True)
    mix_weights = jax.nn.softmax(route_logits, axis=-1)
    picked = answers.reshape(received, model_width)[slot_place].reshape(
        tok_rows, picks, model_width
    )
    mixed_rows = jnp.zeros((tok_rows, model_width), jnp.float32)
    for column in range(picks):
        mixed_rows = mixed_rows + mix_weights[:, column : column + 1] * picked[:, column].astype(
            jnp.float32
        )
    return mixed_rows.astype(jnp.bfloat16)


def remote(src, dst, send_sem, recv_sem, target):
    return pltpu.make_async_remote_copy(
        src_ref=src,
        dst_ref=dst,
        send_sem=send_sem,
        recv_sem=recv_sem,
        device_id={"ep": target},
        device_id_type=pl.DeviceIdType.MESH,
    )


PIECES = len(KINDS)
CELLS = [(p, d, c) for p in range(PIECES) for d in range(4) for c in range(2)]
PARTS = 6


def slots_of(batches):
    filled, table = [0] * PIECES, {}
    for cell, batch in zip(CELLS, batches):
        table[cell] = (batch, filled[batch])
        filled[batch] += 1
    return table


SLOT = (slots_of(END_BATCHES), slots_of(MID_BATCHES))


def at(cell):
    return (cell[0] * 4 + cell[1]) * 2 + cell[2]


def place_of(cell):
    return cell[1] * 2 + cell[2]


def moves(role, cell):
    p, d, c = cell
    first_z = KINDS[p] == 0
    out = []
    if d == 0 and (c == 0 or not first_z):
        if role == 0:
            out.append(("in", 1, (p, 3, c)))
        else:
            out.append(("out", 0, (p, 1, c)))
            out.append(("in", 1, (p, 1, c)))
    elif d > 0 and (c == 0 or not first_z) and role == 1:
        if d == 3:
            out.append(("in", 1, (p, 2, c)))
        else:
            out.append(("out", 0, (p, d + 1, c)))
    if c == 0 and (first_z or d == 0):
        across = ("x", role, (p, d, 1))
        out = out + [across] if first_z else [across] + out
    return out


def fused_kernel(
    n,
    tok_ref,
    ids_hbm,
    logits_hbm,
    wg_hbm,
    wu_hbm,
    wd_hbm,
    out_ref,
    xs,
    wg,
    wu,
    wd,
    ps,
    sib,
    put,
    got_x,
    got_in,
    got_out,
    hid,
    ids_ref,
    logits_ref,
    gates,
    gate_tok,
    gate_col,
    load_sem,
    tok_sem,
    ag_send,
    ag_recv,
    twin_send,
    twin_recv,
    gate_send,
    gate_recv,
    gate_pass,
    sib_send,
    sib_recv,
    rs_send,
    x_recv,
    in_recv,
    out_recv,
):
    tok_rows, width = tok_ref.shape
    rows = tok_rows // PIECES
    ff = wg.shape[1]
    me = lax.axis_index("ep")
    core, chip = me % 2, me // 2
    other = 1 - core
    x, z = chip % 2, chip // 2
    depth = n // 4
    inward = jnp.where(z < depth // 2, 1, -1)
    at_end = jnp.logical_or(z == 0, z == depth - 1)
    at_mid = jnp.logical_not(at_end)
    peers = {
        "in": ((z + inward) * 2 + x) * 2 + core,
        "out": ((z - inward) * 2 + x) * 2 + core,
        "x": (z * 2 + 1 - x) * 2 + core,
        "twin": chip * 2 + other,
    }

    def by_role(end_part, mid_part):
        if end_part is not None:
            pl.when(at_end)(end_part)
        if mid_part is not None:
            pl.when(at_mid)(mid_part)

    barrier = pltpu.get_barrier_semaphore()

    def greet(friend):
        pl.semaphore_signal(
            barrier,
            inc=1,
            device_id={"ep": peers[friend]},
            device_id_type=pl.DeviceIdType.MESH,
        )

    greet("twin")
    greet("x")
    greet("in")
    by_role(None, lambda: greet("out"))

    small_loads = [
        pltpu.make_async_copy(ids_hbm, ids_ref, load_sem.at[3]),
        pltpu.make_async_copy(logits_hbm, logits_ref, load_sem.at[4]),
    ]
    for load in small_loads:
        load.start()

    def chunk(role, cell, whose):
        batch, place = SLOT[role][cell]
        return xs.at[(batch * PIECES + place) * 2 + whose]

    def own_load(role, p):
        return pltpu.make_async_copy(
            tok_ref.at[pl.ds(p * rows, rows)], chunk(role, (p, 0, 0), core), tok_sem.at[p]
        )

    def load_all(role):
        for code in ORDERS[role]:
            if code // 1000 == 0 and code % 100 == 0:
                own_load(role, code // 100).start()

    by_role(lambda: load_all(0), lambda: load_all(1))
    weight_loads = [
        pltpu.make_async_copy(wg_hbm.at[0], wg, load_sem.at[0]),
        pltpu.make_async_copy(wu_hbm.at[0], wu, load_sem.at[1]),
        pltpu.make_async_copy(wd_hbm.at[0], wd, load_sem.at[2]),
    ]
    for load in weight_loads:
        load.start()

    for load in small_loads:
        load.wait()
    logits = logits_ref[...]
    powers = jnp.exp(logits - jnp.max(logits, axis=0, keepdims=True))
    shares = powers / jnp.sum(powers, axis=0, keepdims=True)
    ids = ids_ref[...]
    for expert in range(n):
        gates[core, expert] = jnp.sum(
            jnp.where(ids == expert, shares, 0.0), axis=0, keepdims=True
        )

    by_role(lambda: pl.semaphore_wait(barrier, 3), lambda: pl.semaphore_wait(barrier, 4))

    def ag_copy(role, cell, link, to_role, to_cell):
        return remote(
            chunk(role, cell, core),
            chunk(to_role, to_cell, core),
            ag_send.at[0],
            ag_recv.at[at(to_cell)],
            peers[link],
        )

    def pass_copy(role, cell, whose):
        batch, place = SLOT[role][cell]
        ref = chunk(role, cell, whose)
        return remote(ref, ref, twin_send.at[0], twin_recv.at[batch], peers["twin"])

    def gate_copy(cell, link, to_cell):
        return remote(
            gates.at[place_of(cell) * 2 + core],
            gates.at[place_of(to_cell) * 2 + core],
            gate_send.at[0],
            gate_recv.at[place_of(to_cell)],
            peers[link],
        )

    def gate_twin(cell, whose):
        place = place_of(cell)
        ref = gates.at[place * 2 + whose]
        return remote(ref, ref, gate_send.at[1], gate_pass.at[place], peers["twin"])

    def receive(role, cell):
        p, d, c = cell
        lead = p == 0
        if (d, c) == (0, 0):
            own_load(role, p).wait()
        else:
            if lead:
                gate_copy(cell, "x", cell).wait_recv()
            ag_copy(role, cell, "x", role, cell).wait_recv()
        for link, to_role, to_cell in moves(role, cell):
            if lead:
                gate_copy(cell, link, to_cell).start()
            ag_copy(role, cell, link, to_role, to_cell).start()
        if lead:
            gate_twin(cell, core).start()
        pass_copy(role, cell, core).start()

    def sib_copy(batch, half, whose):
        cols = pl.ds(half * (width // 2), width // 2)
        return remote(
            ps.at[batch, :, whose, :, cols],
            sib.at[batch, :, :, cols],
            sib_send.at[0],
            sib_recv.at[batch],
            peers["twin"],
        )

    sib_seen = (set(), set())
    put_used = [0, 0]

    def send_back(role, cell):
        p, d, c = cell
        first_z = KINDS[p] == 0
        batch, place = SLOT[role][cell]
        if batch not in sib_seen[role]:
            sib_seen[role].add(batch)
            ref = sib.at[batch]
            remote(ref, ref, sib_send.at[0], sib_recv.at[batch], peers["twin"]).wait_recv()
        total = ps[batch, place, core].astype(jnp.float32) + sib[batch, place].astype(jnp.float32)
        inbox = []
        if c == 0 and (first_z or d == 0):
            inbox.append((got_x, x_recv, p * 4 + d))
        if c == 0 or not first_z:
            if d == 0 or (d == 3 and role == 1):
                inbox.append((got_in, in_recv, (p * 2 + d // 3) * 2 + c))
            if role == 1 and d < 3:
                inbox.append((got_out, out_recv, (p * 3 + d) * 2 + c))
        for buffer, sem, index in inbox:
            ref = buffer.at[index]
            remote(ref, ref, rs_send.at[0], sem.at[index], peers["x"]).wait_recv()
            total = total + buffer[index].astype(jnp.float32)
        total = total.astype(jnp.bfloat16)
        if c == 1 and (first_z or d == 0):
            link, buffer, sem, index = "x", got_x, x_recv, p * 4 + d
        elif d == 0:
            out_ref[pl.ds(p * rows, rows), :] = total
            return
        elif role == 0:
            link, buffer, sem, index = "in", got_out, out_recv, (p * 3 + d - 1) * 2 + c
        elif d == 3:
            link, buffer, sem, index = "out", got_in, in_recv, p * 4 + c
        else:
            link, buffer, sem, index = "in", got_in, in_recv, (p * 2 + d - 1) * 2 + c
        slot = put_used[role]
        put_used[role] += 1
        put[slot] = total
        remote(put.at[slot], buffer.at[index], rs_send.at[0], sem.at[index], peers[link]).start()

    ff_tile = ff // 4
    out_tile = width // 4

    def hidden_part(batch, first, last):
        def body(j, carry):
            rows_in = xs[pl.ds(batch * 2 * PIECES, 2 * PIECES)].reshape(2 * tok_rows, width)
            cols = pl.ds(pl.multiple_of(j * ff_tile, ff_tile), ff_tile)
            gate = jnp.dot(rows_in, wg[:, cols], preferred_element_type=jnp.float32)
            up = jnp.dot(rows_in, wu[:, cols], preferred_element_type=jnp.float32)
            hid[:, cols] = (gate / (1.0 + jnp.exp(-gate)) * up).astype(jnp.bfloat16)
            return carry

        lax.fori_loop(first, last, body, 0)

    def answer_part(batch, first, last):
        def body(j, carry):
            cols = pl.ds(pl.multiple_of(j * out_tile, out_tile), out_tile)
            answer = jnp.dot(hid[...], wd[:, cols], preferred_element_type=jnp.float32)
            scale = jnp.concatenate([gate_col[...]] * (out_tile // 128), axis=1)
            ps[batch, :, :, :, cols] = (
                (answer * scale).astype(jnp.bfloat16).reshape(PIECES, 2, rows, out_tile)
            )
            return carry

        lax.fori_loop(first, last, body, 0)

    gates_seen = (set(), set())

    def gate_fill(role, batch):
        for cell in CELLS:
            if SLOT[role][cell][0] != batch:
                continue
            p, d, c = cell
            source = place_of(cell)
            if source not in gates_seen[role]:
                gates_seen[role].add(source)
                gate_twin((0, d, c), other).wait_recv()
                for whose in range(2):
                    row = gates[source * 2 + whose, me]
                    gate_tok[source * 2 + whose] = jnp.broadcast_to(row, (128, tok_rows)).T
            for whose in range(2):
                first = (SLOT[role][cell][1] * 2 + whose) * rows
                gate_col[pl.ds(first, rows), :] = gate_tok[source * 2 + whose, pl.ds(p * rows, rows), :]

    def compute(batch, first, last):
        if first == 0:
            ref = xs.at[pl.ds(0, PIECES)]
            remote(ref, ref, twin_send.at[0], twin_recv.at[batch], peers["twin"]).wait_recv()
            if batch == 0:
                weight_loads[0].wait()
                weight_loads[1].wait()
        if first < 4:
            hidden_part(batch, first, min(last, 4))
        if first <= 4 < last:
            by_role(lambda: gate_fill(0, batch), lambda: gate_fill(1, batch))
            if batch == 0:
                weight_loads[2].wait()
        for part in range(max(first, 4), last):
            answer_part(batch, (part - 4) * 2, (part - 3) * 2)
            sib_copy(batch, part - 4, other).start()

    def events(role, codes):
        if not codes:
            return None

        def run():
            for code in codes:
                cell = (code // 100 % 10, code // 10 % 10, code % 10)
                if code < 1000:
                    receive(role, cell)
                else:
                    send_back(role, cell)

        return run

    plans = []
    for order in ORDERS:
        plan, now = [], []
        for code in order:
            if code // 1000 == 1:
                plan.append((now, code))
                now = []
            else:
                now.append(code)
        plan.append((now, None))
        plans.append(plan)

    waiting = None
    for (end_codes, code), (mid_codes, mid_code) in zip(*plans):
        assert code == mid_code
        batch, part = (None, None) if code is None else (code // 100 % 10, code // 10 % 10)
        if waiting is not None and (end_codes or mid_codes or batch != waiting[0]):
            compute(*waiting)
            waiting = None
        by_role(events(0, end_codes), events(1, mid_codes))
        if code is not None:
            waiting = (batch, part, part + 1) if waiting is None else (batch, waiting[1], part + 1)

    def finish(role):
        sent = sum(len(moves(role, cell)) for cell in CELLS)
        ref = xs.at[pl.ds(0, sent)]
        remote(ref, ref, ag_send.at[0], ag_recv.at[0], peers["x"]).wait_send()
        sent = sum(len(moves(role, cell)) for cell in CELLS if cell[0] == 0)
        ref = gates.at[pl.ds(0, sent)]
        remote(ref, ref, gate_send.at[0], gate_recv.at[0], peers["x"]).wait_send()

    by_role(lambda: finish(0), lambda: finish(1))
    ref = xs.at[pl.ds(0, len(CELLS))]
    remote(ref, ref, twin_send.at[0], twin_recv.at[0], peers["twin"]).wait_send()
    ref = gates.at[pl.ds(0, 8)]
    remote(ref, ref, gate_send.at[1], gate_pass.at[0], peers["twin"]).wait_send()
    remote(sib, sib, sib_send.at[0], sib_recv.at[0], peers["twin"]).wait_send()
    assert put_used == [put.shape[0]] * 2
    remote(put, put, rs_send.at[0], x_recv.at[0], peers["x"]).wait_send()


def fused_scratch(n, tok_rows, width, ff, picks):
    bf16, f32 = jnp.bfloat16, jnp.float32
    rows = tok_rows // PIECES
    chunk = (rows, width)
    buffers = [
        ((PIECES * 16,) + chunk, bf16),
        ((width, ff), bf16),
        ((width, ff), bf16),
        ((ff, width), bf16),
        ((PIECES, 8, 2) + chunk, bf16),
        ((PIECES, 8) + chunk, bf16),
        ((PIECES * 7,) + chunk, bf16),
        ((PIECES * 4,) + chunk, bf16),
        ((PIECES * 4,) + chunk, bf16),
        ((PIECES * 6,) + chunk, bf16),
        ((2 * tok_rows, ff), bf16),
        ((picks, tok_rows), jnp.int32),
        ((picks, tok_rows), f32),
        ((16, n, 1, tok_rows), f32),
        ((16, tok_rows, 128), f32),
        ((2 * tok_rows, 128), f32),
    ]
    sems = [5, PIECES, 1, PIECES * 8, 1, PIECES, 2, 8, 8, 1, PIECES, 1]
    sems += [PIECES * 4, PIECES * 4, PIECES * 6]
    size = 0
    for shape, kind in buffers:
        count = jnp.dtype(kind).itemsize
        for extent in shape:
            count = count * extent
        size = size + count
    scratch = [pltpu.VMEM(shape, kind) for shape, kind in buffers]
    return scratch + [pltpu.SemaphoreType.DMA((count,)) for count in sems], size


def fused_device(tokens, expert_ids, route_logits, w_gate, w_up, w_down):
    n = lax.axis_size("ep")
    tok_rows, width = tokens.shape
    ff = w_gate.shape[2]
    scratch, size = fused_scratch(n, tok_rows, width, ff, expert_ids.shape[1])
    anywhere, vmem = pl.BlockSpec(memory_space=pl.ANY), pl.BlockSpec(memory_space=pltpu.VMEM)
    return pl.pallas_call(
        functools.partial(fused_kernel, n),
        out_shape=pltpu.VMEM((tok_rows, width), jnp.bfloat16),
        in_specs=[anywhere] * 6,
        out_specs=vmem,
        scratch_shapes=scratch,
        compiler_params=pltpu.CompilerParams(
            collective_id=0, has_side_effects=True, vmem_limit_bytes=VMEM_BYTES
        ),
    )(tokens, expert_ids.T, route_logits.T, w_gate, w_up, w_down)


def layer(tokens, expert_ids, route_logits, w_gate, w_up, w_down):
    n = lax.axis_size("ep")
    tok_rows, width = tokens.shape
    ff = w_gate.shape[2]
    size = fused_scratch(n, tok_rows, width, ff, expert_ids.shape[1])[1]
    fits = size + 8 * tok_rows * width < VMEM_BYTES and width % 512 == 0 and ff % 512 == 0
    if fits and n == 16 and tok_rows == 16 * PIECES:
        return fused_device(tokens, expert_ids, route_logits, w_gate, w_up, w_down)
    return per_device(tokens, expert_ids, route_logits, w_gate, w_up, w_down)


def solution(mesh):
    in_specs = (
        P(("dp", "ep"), None),
        P(("dp", "ep"), None),
        P(("dp", "ep"), None),
        P("ep", None, None),
        P("ep", None, None),
        P("ep", None, None),
    )
    out_specs = P(("dp", "ep"), None)
    return jax.shard_map(
        layer, mesh=mesh, in_specs=in_specs, out_specs=out_specs, check_vma=False
    )
```

```python
import functools

import jax
import jax.numpy as jnp
from jax import lax
from jax.experimental import pallas as pl
from jax.experimental.pallas import tpu as pltpu
from jax.sharding import PartitionSpec as P

VMEM_BYTES = 63 * 1024 * 1024

GATHER_X = (0, 0, 1, 1, 1, 1, 0, 0, 0, 0)
SUM_Z = (1, 0, 0, 0, 0, 1, 0, 0, 1, 1)
PARTS = (0, 1, 2, 3, 4, 4, 5, 6, 6, 7)
END_BATCHES = (
    1, 1, 0, 0, 0, 1, 2, 3, 0, 4, 5, 6, 4, 5, 4, 3,
    7, 2, 6, 6, 5, 6, 3, 4, 7, 3, 7, 7, 6, 6, 6, 3,
    5, 2, 2, 0, 0, 2, 1, 2, 7, 3, 5, 2, 5, 5, 5, 4,
    7, 7, 0, 0, 1, 1, 4, 4, 6, 7, 1, 1, 4, 3, 2, 3,
)
MID_BATCHES = (
    2, 3, 2, 1, 1, 3, 1, 5, 7, 6, 5, 5, 4, 3, 5, 2,
    7, 6, 7, 6, 5, 3, 1, 4, 4, 5, 7, 6, 5, 4, 0, 1,
    4, 7, 0, 0, 6, 6, 0, 2, 4, 7, 7, 3, 6, 3, 2, 2,
    5, 1, 0, 1, 3, 2, 3, 0, 7, 0, 0, 4, 4, 2, 6, 1,
)
END_ORDER = (
    500, 0, 400, 800, 900, 510, 501, 700, 1, 10, 410, 401, 100, 801, 710, 901,
    810, 701, 910, 520, 420, 11, 300, 101, 20, 511, 711, 811, 820, 411, 200, 911,
    530, 10000, 720, 10010, 301, 600, 10020, 21, 430, 10030, 521, 30, 821, 10040, 421, 10050,
    531, 201, 431, 721, 830, 20520, 601, 20411, 20511, 20711, 20020, 10100, 920, 10110, 31, 20810,
    20010, 610, 10120, 831, 10130, 930, 20011, 10140, 730, 10150, 921, 20710, 20811, 230, 611, 20530,
    130, 20021, 20721, 10200, 931, 331, 20821, 731, 10210, 20911, 10220, 630, 20820, 10230, 620, 131,
    20910, 10240, 10250, 110, 20720, 10300, 10310, 631, 20510, 20030, 20201, 20421, 231, 10320, 210, 20930,
    621, 20611, 10330, 10340, 120, 111, 20531, 20521, 10350, 310, 20431, 20410, 20401, 10400, 220, 20420,
    10410, 20131, 20031, 20921, 20331, 211, 10420, 10430, 121, 330, 20301, 20931, 10440, 10450, 311, 20430,
    20601, 10500, 320, 10510, 20130, 20830, 20731, 20231, 10520, 221, 20831, 10530, 20631, 20920, 321, 10540,
    20101, 10550, 10600, 20730, 10610, 10620, 20230, 20121, 20621, 20610, 10630, 10640, 20630, 10650, 20001, 10700,
    10710, 20330, 20221, 20120, 20321, 10720, 10730, 20620, 20111, 10740, 20100, 20000, 10750, 20211, 20220, 20311,
    20320, 20901, 20110, 20701, 20501, 20210, 20801, 20200, 20310, 20600, 20900, 20300, 20700, 20500, 20400, 20800,
)
MID_ORDER = (
    500, 0, 400, 800, 700, 900, 510, 530, 1, 30, 410, 10, 801, 430, 701, 501,
    810, 830, 901, 401, 520, 531, 31, 431, 710, 20, 730, 11, 930, 811, 420, 831,
    511, 130, 711, 411, 521, 330, 21, 421, 731, 820, 910, 931, 230, 10000, 600, 131,
    10010, 821, 920, 10020, 331, 10030, 720, 630, 911, 10040, 220, 10050, 601, 120, 10100, 921,
    231, 10110, 321, 721, 20731, 20510, 20411, 10120, 620, 10130, 631, 10140, 610, 121, 10150, 10200,
    100, 10210, 10220, 20331, 20701, 221, 621, 10230, 200, 611, 10240, 10250, 101, 110, 20011, 10300,
    300, 10310, 20010, 10320, 20131, 210, 10330, 20811, 20721, 201, 10340, 20711, 10350, 320, 20631, 111,
    20810, 10400, 20431, 301, 10410, 20001, 20020, 10420, 310, 10430, 20710, 20121, 10440, 20621, 20511, 211,
    10450, 10500, 311, 20221, 20410, 10510, 20030, 20021, 20231, 20000, 20920, 10520, 10530, 20611, 20911, 10540,
    10550, 20921, 20321, 10600, 20801, 10610, 20301, 20031, 20700, 20120, 10620, 20820, 10630, 20901, 20821, 10640,
    20111, 20910, 20931, 10650, 20800, 20720, 10700, 20130, 10710, 20101, 20421, 20520, 20521, 20220, 20930, 20830,
    20201, 10720, 20831, 10730, 20211, 10740, 20730, 20620, 10750, 20531, 20530, 20311, 20320, 20420, 20601, 20230,
    20900, 20110, 20501, 20401, 20630, 20610, 20330, 20210, 20430, 20310, 20500, 20100, 20400, 20600, 20200, 20300,
)
ORDERS = (END_ORDER, MID_ORDER)


def expert_ffn(rows, gate_weight, up_weight, down_weight):
    gate = jnp.dot(rows, gate_weight, preferred_element_type=jnp.float32)
    up_part = jnp.dot(rows, up_weight, preferred_element_type=jnp.float32)
    hidden = (jax.nn.silu(gate) * up_part).astype(jnp.bfloat16)
    return jnp.dot(hidden, down_weight, preferred_element_type=jnp.float32).astype(jnp.bfloat16)


def blockwise(rows, live_rows, weights):
    turns = (live_rows + 127) // 128

    def step(block_index, result):
        first_row = block_index * 128
        block_rows = lax.dynamic_slice_in_dim(rows, first_row, 128, 0)
        answer = expert_ffn(block_rows, weights[0], weights[1], weights[2])
        return lax.dynamic_update_slice_in_dim(result, answer, first_row, 0)

    return lax.fori_loop(jnp.int32(0), turns, step, jnp.zeros(rows.shape, jnp.bfloat16))


def per_device(tokens, expert_ids, route_logits, w_gate, w_up, w_down):
    tok_rows, model_width = tokens.shape
    picks = expert_ids.shape[1]
    experts = lax.axis_size("ep")
    capacity = min(tok_rows, 3 * tok_rows * picks // (2 * experts))
    row_quota = tok_rows * picks
    received = experts * capacity
    spill_count = (max(received - row_quota, 128) + 127) // 128 * 128
    length = row_quota + spill_count
    flat_ids = expert_ids.reshape(-1)
    one_hot = (flat_ids[:, None] == jnp.arange(experts, dtype=jnp.int32)[None, :]).astype(jnp.int32)
    earlier = jnp.cumsum(one_hot, axis=0) - one_hot
    slot_rank = jnp.sum(earlier * one_hot, axis=1)
    counts = jnp.sum(one_hot, axis=0)
    slot_place = flat_ids * capacity + slot_rank
    source_row = jnp.arange(row_quota, dtype=jnp.int32) // picks
    slot_token = jnp.full((received,), tok_rows, jnp.int32).at[slot_place].set(source_row)
    padded_tokens = jnp.concatenate([tokens, jnp.zeros((1, model_width), tokens.dtype)], 0)
    outgoing = padded_tokens[slot_token].reshape(experts, capacity, model_width)
    all_counts = lax.all_gather(counts, "ep", axis=0, tiled=True).reshape(experts, experts)
    own_index = lax.axis_index("ep")
    from_sources = lax.dynamic_index_in_dim(all_counts, own_index, 1, keepdims=False)
    incoming = lax.all_to_all(outgoing, "ep", split_axis=0, concat_axis=0, tiled=True)
    offsets = jnp.cumsum(from_sources) - from_sources
    live_rows = jnp.sum(from_sources)
    slot_numbers = jnp.arange(capacity, dtype=jnp.int32)
    live_slot = slot_numbers[None, :] < from_sources[:, None]
    position = jnp.where(live_slot, offsets[:, None] + slot_numbers[None, :], length).reshape(-1)
    gather_order = (
        jnp.full((length,), received, jnp.int32)
        .at[position]
        .set(jnp.arange(received, dtype=jnp.int32), mode="drop")
    )
    flat_incoming = jnp.concatenate(
        [incoming.reshape(received, model_width), jnp.zeros((1, model_width), jnp.bfloat16)], 0
    )
    packed = flat_incoming[gather_order]
    own_weights = (w_gate[0], w_up[0], w_down[0])
    results = blockwise(packed, live_rows, own_weights)
    results_ext = jnp.concatenate([results, jnp.zeros((1, model_width), jnp.bfloat16)], 0)
    outgoing_back = results_ext[position].reshape(experts, capacity, model_width)
    answers = lax.all_to_all(outgoing_back, "ep", split_axis=0, concat_axis=0, tiled=True)
    mix_weights = jax.nn.softmax(route_logits, axis=-1)
    picked = answers.reshape(received, model_width)[slot_place].reshape(
        tok_rows, picks, model_width
    )
    mixed_rows = jnp.zeros((tok_rows, model_width), jnp.float32)
    for column in range(picks):
        mixed_rows = mixed_rows + mix_weights[:, column : column + 1] * picked[:, column].astype(
            jnp.float32
        )
    return mixed_rows.astype(jnp.bfloat16)


def remote(src, dst, send_sem, recv_sem, target):
    return pltpu.make_async_remote_copy(
        src_ref=src,
        dst_ref=dst,
        send_sem=send_sem,
        recv_sem=recv_sem,
        device_id={"ep": target},
        device_id_type=pl.DeviceIdType.MESH,
    )


SENDS = len(GATHER_X)
PIECES = len(END_BATCHES) // 8
CELLS = [(h, d, c) for h in range(SENDS) for d in range(4) for c in range(2)]


def slots_of(batches):
    filled, table = [0] * PIECES, {}
    places = [(piece, d, c) for piece in range(PIECES) for d in range(4) for c in range(2)]
    for (piece, d, c), batch in zip(places, batches):
        for p in range(SENDS):
            if PARTS[p] == piece:
                table[p, d, c] = (batch, filled[batch])
        filled[batch] += 1
    return table


SLOT = (slots_of(END_BATCHES), slots_of(MID_BATCHES))


def at(cell):
    return (cell[0] * 4 + cell[1]) * 2 + cell[2]


def place_of(cell):
    return cell[1] * 2 + cell[2]


def moves(role, cell):
    p, d, c = cell
    first_z = not GATHER_X[p]
    out = []
    if d == 0 and (c == 0 or not first_z):
        if role == 0:
            out.append(("in", 1, (p, 3, c)))
        else:
            out.append(("out", 0, (p, 1, c)))
            out.append(("in", 1, (p, 1, c)))
    elif d > 0 and (c == 0 or not first_z) and role == 1:
        if d == 3:
            out.append(("in", 1, (p, 2, c)))
        else:
            out.append(("out", 0, (p, d + 1, c)))
    if c == 0 and (first_z or d == 0):
        across = ("x", role, (p, d, 1))
        out = out + [across] if first_z else [across] + out
    return out


def fused_kernel(
    n,
    tok_ref,
    ids_hbm,
    logits_hbm,
    wg_hbm,
    wu_hbm,
    wd_hbm,
    out_ref,
    xs,
    wg,
    wu,
    wd,
    ps,
    sib,
    put,
    got_x,
    got_in,
    got_out,
    hid,
    ids_ref,
    logits_ref,
    gates,
    gate_tok,
    gate_col,
    load_sem,
    tok_sem,
    ag_send,
    ag_recv,
    twin_send,
    twin_recv,
    gate_send,
    gate_recv,
    gate_pass,
    sib_send,
    sib_recv,
    rs_send,
    x_recv,
    in_recv,
    out_recv,
):
    tok_rows, width = tok_ref.shape
    rows = tok_rows // PIECES
    ff = wg.shape[1]
    ff_tile = ff // 4
    out_tile = width // 4
    me = lax.axis_index("ep")
    core, chip = me % 2, me // 2
    other = 1 - core
    x, z = chip % 2, chip // 2
    depth = n // 4
    inward = jnp.where(z < depth // 2, 1, -1)
    at_end = jnp.logical_or(z == 0, z == depth - 1)
    at_mid = jnp.logical_not(at_end)
    peers = {
        "in": ((z + inward) * 2 + x) * 2 + other,
        "out": ((z - inward) * 2 + x) * 2 + other,
        "x": (z * 2 + 1 - x) * 2 + other,
        "twin": chip * 2 + other,
    }

    def by_role(end_part, mid_part):
        if end_part is not None:
            pl.when(at_end)(end_part)
        if mid_part is not None:
            pl.when(at_mid)(mid_part)

    barrier = pltpu.get_barrier_semaphore()

    def greet(friend):
        pl.semaphore_signal(
            barrier,
            inc=1,
            device_id={"ep": peers[friend]},
            device_id_type=pl.DeviceIdType.MESH,
        )

    greet("twin")
    greet("x")
    greet("in")
    by_role(None, lambda: greet("out"))

    small_loads = [
        pltpu.make_async_copy(ids_hbm, ids_ref, load_sem.at[3]),
        pltpu.make_async_copy(logits_hbm, logits_ref, load_sem.at[4]),
    ]
    for load in small_loads:
        load.start()

    def cols_of(cell):
        piece = PARTS[cell[0]]
        part_width = width // PARTS.count(piece)
        return pl.ds((cell[0] - PARTS.index(piece)) * part_width, part_width)

    def chunk(role, cell, whose):
        batch, place = SLOT[role][cell]
        return xs.at[(batch * PIECES + place) * 2 + whose, :, cols_of(cell)]

    def own_load(role, p):
        return pltpu.make_async_copy(
            tok_ref.at[pl.ds(PARTS[p] * rows, rows), cols_of((p, 0, 0))],
            chunk(role, (p, 0, 0), core),
            tok_sem.at[p],
        )

    def load_all(role):
        for code in ORDERS[role]:
            if code // 10000 == 0 and code % 100 == 0:
                own_load(role, code // 100).start()

    by_role(lambda: load_all(0), lambda: load_all(1))
    weight_loads = [
        pltpu.make_async_copy(wg_hbm.at[0], wg, load_sem.at[0]),
        pltpu.make_async_copy(wu_hbm.at[0], wu, load_sem.at[1]),
        pltpu.make_async_copy(wd_hbm.at[0], wd, load_sem.at[2]),
    ]
    for load in weight_loads:
        load.start()

    def own_gates():
        for load in small_loads:
            load.wait()
        logits = logits_ref[...]
        powers = jnp.exp(logits - jnp.max(logits, axis=0, keepdims=True))
        shares = powers / jnp.sum(powers, axis=0, keepdims=True)
        ids = ids_ref[...]
        for expert in range(n):
            gates[core, expert] = jnp.sum(
                jnp.where(ids == expert, shares, 0.0), axis=0, keepdims=True
            )

    by_role(lambda: pl.semaphore_wait(barrier, 3), lambda: pl.semaphore_wait(barrier, 4))

    def ag_copy(role, cell, link, to_role, to_cell):
        return remote(
            chunk(role, cell, core),
            chunk(to_role, to_cell, other),
            ag_send.at[0],
            ag_recv.at[at(to_cell)],
            peers[link],
        )

    def pass_copy(role, cell, whose):
        batch, place = SLOT[role][cell]
        ref = chunk(role, cell, whose)
        return remote(ref, ref, twin_send.at[0], twin_recv.at[batch], peers["twin"])

    def gate_copy(cell, link, to_cell):
        return remote(
            gates.at[place_of(cell) * 2 + core],
            gates.at[place_of(to_cell) * 2 + other],
            gate_send.at[0],
            gate_recv.at[place_of(to_cell)],
            peers[link],
        )

    def gate_twin(cell, whose):
        place = place_of(cell)
        ref = gates.at[place * 2 + whose]
        return remote(ref, ref, gate_send.at[1], gate_pass.at[place], peers["twin"])

    def receive(role, cell):
        p, d, c = cell
        lead = p == 0
        if (d, c) == (0, 0):
            if lead:
                own_gates()
            own_load(role, p).wait()
        else:
            if lead:
                gate_copy(cell, "x", cell).wait_recv()
            ag_copy(role, cell, "x", role, cell).wait_recv()
        for link, to_role, to_cell in moves(role, cell):
            if lead:
                gate_copy(cell, link, to_cell).start()
            ag_copy(role, cell, link, to_role, to_cell).start()
        if lead:
            gate_twin(cell, core).start()
        pass_copy(role, cell, core).start()

    def sib_copy(batch, part, whose):
        cols = pl.ds(pl.multiple_of(part * out_tile, out_tile), out_tile)
        return remote(
            ps.at[batch, :, whose, :, cols],
            sib.at[batch, :, :, cols],
            sib_send.at[0],
            sib_recv.at[batch],
            peers["twin"],
        )

    sib_seen = (set(), set())
    put_used = [0, 0]

    def send_back(role, cell):
        p, d, c = cell
        first_z = not SUM_Z[p]
        batch, place = SLOT[role][cell]
        cols = cols_of(cell)
        if batch not in sib_seen[role]:
            sib_seen[role].add(batch)
            ref = sib.at[batch]
            remote(ref, ref, sib_send.at[0], sib_recv.at[batch], peers["twin"]).wait_recv()
        total = ps[batch, place, core, :, cols].astype(jnp.float32)
        total = total + sib[batch, place, :, cols].astype(jnp.float32)
        inbox = []
        if c == 0 and (first_z or d == 0):
            inbox.append((got_x, x_recv, p * 4 + d))
        if c == 0 or not first_z:
            if d == 0 or (d == 3 and role == 1):
                inbox.append((got_in, in_recv, (p * 2 + d // 3) * 2 + c))
            if role == 1 and d < 3:
                inbox.append((got_out, out_recv, (p * 3 + d) * 2 + c))
        for buffer, sem, index in inbox:
            ref = buffer.at[index, :, pl.ds(0, cols.size)]
            remote(ref, ref, rs_send.at[0], sem.at[index], peers["x"]).wait_recv()
            total = total + buffer[index, :, pl.ds(0, cols.size)].astype(jnp.float32)
        total = total.astype(jnp.bfloat16)
        if c == 1 and (first_z or d == 0):
            link, buffer, sem, index = "x", got_x, x_recv, p * 4 + d
        elif d == 0:
            out_ref[pl.ds(PARTS[p] * rows, rows), cols] = total
            return
        elif role == 0:
            link, buffer, sem, index = "in", got_out, out_recv, (p * 3 + d - 1) * 2 + c
        elif d == 3:
            link, buffer, sem, index = "out", got_in, in_recv, p * 4 + c
        else:
            link, buffer, sem, index = "in", got_in, in_recv, (p * 2 + d - 1) * 2 + c
        slot = put_used[role]
        put_used[role] += 1
        used = pl.ds(0, cols.size)
        put[slot, :, used] = total
        remote(
            put.at[slot, :, used],
            buffer.at[index, :, used],
            rs_send.at[0],
            sem.at[index],
            peers[link],
        ).start()

    def hidden_part(batch, first, last):
        def body(j, carry):
            rows_in = xs[pl.ds(batch * 2 * PIECES, 2 * PIECES)].reshape(2 * tok_rows, width)
            cols = pl.ds(pl.multiple_of(j * ff_tile, ff_tile), ff_tile)
            gate = jnp.dot(rows_in, wg[:, cols], preferred_element_type=jnp.float32)
            up = jnp.dot(rows_in, wu[:, cols], preferred_element_type=jnp.float32)
            hid[:, cols] = (gate / (1.0 + jnp.exp(-gate)) * up).astype(jnp.bfloat16)
            return carry

        lax.fori_loop(first, last, body, 0)

    def answer_part(batch, first, last):
        def body(j, carry):
            cols = pl.ds(pl.multiple_of(j * out_tile, out_tile), out_tile)
            answer = jnp.dot(hid[...], wd[:, cols], preferred_element_type=jnp.float32)
            scale = jnp.concatenate([gate_col[...]] * (out_tile // 128), axis=1)
            ps[batch, :, :, :, cols] = (
                (answer * scale).astype(jnp.bfloat16).reshape(PIECES, 2, rows, out_tile)
            )
            sib_copy(batch, j, other).start()
            return carry

        lax.fori_loop(first, last, body, 0)

    gates_seen = (set(), set())

    def gate_fill(role, batch):
        for cell in CELLS:
            p, d, c = cell
            if SLOT[role][cell][0] != batch or PARTS.index(PARTS[p]) != p:
                continue
            source = place_of(cell)
            if source not in gates_seen[role]:
                gates_seen[role].add(source)
                gate_twin((0, d, c), other).wait_recv()
                for whose in range(2):
                    row = gates[source * 2 + whose, me]
                    gate_tok[source * 2 + whose] = jnp.broadcast_to(row, (128, tok_rows)).T
            for whose in range(2):
                first = (SLOT[role][cell][1] * 2 + whose) * rows
                gate_col[pl.ds(first, rows), :] = gate_tok[
                    source * 2 + whose, pl.ds(PARTS[p] * rows, rows), :
                ]

    def compute(batch, first, last):
        if first == 0:
            ref = xs.at[pl.ds(0, PIECES)]
            remote(ref, ref, twin_send.at[0], twin_recv.at[batch], peers["twin"]).wait_recv()
            if batch == 0:
                weight_loads[0].wait()
                weight_loads[1].wait()
        if first < 4:
            hidden_part(batch, first, min(last, 4))
        if first <= 4 < last:
            by_role(lambda: gate_fill(0, batch), lambda: gate_fill(1, batch))
            if batch == 0:
                weight_loads[2].wait()
        if last > 4:
            answer_part(batch, max(first, 4) * 2 - 8, last * 2 - 8)

    def events(role, codes):
        if not codes:
            return None

        def run():
            for code in codes:
                cell = (code // 100 % 100, code // 10 % 10, code % 10)
                if code < 10000:
                    receive(role, cell)
                else:
                    send_back(role, cell)

        return run

    plans = []
    for order in ORDERS:
        plan, now = [], []
        for code in order:
            if code // 10000 == 1:
                plan.append((now, code))
                now = []
            else:
                now.append(code)
        plan.append((now, None))
        plans.append(plan)

    waiting = None
    for (end_codes, code), (mid_codes, mid_code) in zip(*plans):
        assert code == mid_code
        batch, part = (None, None) if code is None else (code // 100 % 100, code // 10 % 10)
        if waiting is not None and (end_codes or mid_codes or batch != waiting[0]):
            compute(*waiting)
            waiting = None
        by_role(events(0, end_codes), events(1, mid_codes))
        if code is not None:
            waiting = (batch, part, part + 1) if waiting is None else (batch, waiting[1], part + 1)

    def finish(role):
        sent = sum(len(moves(role, cell)) * 2 // PARTS.count(PARTS[cell[0]]) for cell in CELLS)
        ref = xs.at[pl.ds(0, sent // 2)]
        remote(ref, ref, ag_send.at[0], ag_recv.at[0], peers["x"]).wait_send()
        sent = sum(len(moves(role, cell)) for cell in CELLS if cell[0] == 0)
        ref = gates.at[pl.ds(0, sent)]
        remote(ref, ref, gate_send.at[0], gate_recv.at[0], peers["x"]).wait_send()

    by_role(lambda: finish(0), lambda: finish(1))
    ref = xs.at[pl.ds(0, len(END_BATCHES))]
    remote(ref, ref, twin_send.at[0], twin_recv.at[0], peers["twin"]).wait_send()
    ref = gates.at[pl.ds(0, 8)]
    remote(ref, ref, gate_send.at[1], gate_pass.at[0], peers["twin"]).wait_send()
    remote(sib, sib, sib_send.at[0], sib_recv.at[0], peers["twin"]).wait_send()
    assert put_used == [SENDS * 7] * 2
    ref = put.at[pl.ds(0, PIECES * 7)]
    remote(ref, ref, rs_send.at[0], x_recv.at[0], peers["x"]).wait_send()


def fused_scratch(n, tok_rows, width, ff, picks):
    bf16, f32 = jnp.bfloat16, jnp.float32
    rows = tok_rows // PIECES
    chunk = (rows, width)
    buffers = [
        ((PIECES * 16,) + chunk, bf16),
        ((width, ff), bf16),
        ((width, ff), bf16),
        ((ff, width), bf16),
        ((PIECES, 8, 2) + chunk, bf16),
        ((PIECES, 8) + chunk, bf16),
        ((SENDS * 7,) + chunk, bf16),
        ((SENDS * 4,) + chunk, bf16),
        ((SENDS * 4,) + chunk, bf16),
        ((SENDS * 6,) + chunk, bf16),
        ((2 * tok_rows, ff), bf16),
        ((picks, tok_rows), jnp.int32),
        ((picks, tok_rows), f32),
        ((16, n, 1, tok_rows), f32),
        ((16, tok_rows, 128), f32),
        ((2 * tok_rows, 128), f32),
    ]
    sems = [5, SENDS, 1, SENDS * 8, 1, PIECES, 2, 8, 8, 1, PIECES, 1]
    sems += [SENDS * 4, SENDS * 4, SENDS * 6]
    size = 0
    for shape, kind in buffers:
        count = jnp.dtype(kind).itemsize
        for extent in shape:
            count = count * extent
        size = size + count
    scratch = [pltpu.VMEM(shape, kind) for shape, kind in buffers]
    return scratch + [pltpu.SemaphoreType.DMA((count,)) for count in sems], size


def fused_device(tokens, expert_ids, route_logits, w_gate, w_up, w_down):
    n = lax.axis_size("ep")
    tok_rows, width = tokens.shape
    ff = w_gate.shape[2]
    scratch, size = fused_scratch(n, tok_rows, width, ff, expert_ids.shape[1])
    anywhere, vmem = pl.BlockSpec(memory_space=pl.ANY), pl.BlockSpec(memory_space=pltpu.VMEM)
    return pl.pallas_call(
        functools.partial(fused_kernel, n),
        out_shape=pltpu.VMEM((tok_rows, width), jnp.bfloat16),
        in_specs=[anywhere] * 6,
        out_specs=vmem,
        scratch_shapes=scratch,
        compiler_params=pltpu.CompilerParams(
            collective_id=0, has_side_effects=True, vmem_limit_bytes=VMEM_BYTES
        ),
    )(tokens, expert_ids.T, route_logits.T, w_gate, w_up, w_down)


def layer(tokens, expert_ids, route_logits, w_gate, w_up, w_down):
    n = lax.axis_size("ep")
    tok_rows, width = tokens.shape
    ff = w_gate.shape[2]
    size = fused_scratch(n, tok_rows, width, ff, expert_ids.shape[1])[1]
    fits = size + 8 * tok_rows * width < VMEM_BYTES and width % 512 == 0 and ff % 512 == 0
    if fits and n == 16 and tok_rows == 16 * PIECES:
        return fused_device(tokens, expert_ids, route_logits, w_gate, w_up, w_down)
    return per_device(tokens, expert_ids, route_logits, w_gate, w_up, w_down)


def solution(mesh):
    in_specs = (
        P(("dp", "ep"), None),
        P(("dp", "ep"), None),
        P(("dp", "ep"), None),
        P("ep", None, None),
        P("ep", None, None),
        P("ep", None, None),
    )
    out_specs = P(("dp", "ep"), None)
    return jax.shard_map(
        layer, mesh=mesh, in_specs=in_specs, out_specs=out_specs, check_vma=False
    )
```

```python
import functools

import jax
import jax.numpy as jnp
from jax import lax
from jax.experimental import pallas as pl
from jax.experimental.pallas import tpu as pltpu
from jax.sharding import PartitionSpec as P

VMEM_BYTES = 63 * 1024 * 1024

GATHER_X = (0, 0, 1, 1, 1, 1, 0, 0, 0, 0)
SUM_Z = (1, 0, 0, 0, 0, 1, 0, 0, 1, 1)
PARTS = (0, 1, 2, 3, 4, 4, 5, 6, 6, 7)
END_BATCHES = (
    1, 1, 0, 0, 0, 1, 2, 3, 0, 4, 5, 6, 4, 5, 4, 3,
    7, 2, 6, 6, 5, 6, 3, 4, 7, 3, 7, 7, 6, 6, 6, 3,
    5, 2, 2, 0, 0, 2, 1, 2, 7, 3, 5, 2, 5, 5, 5, 4,
    7, 7, 0, 0, 1, 1, 4, 4, 6, 7, 1, 1, 4, 3, 2, 3,
)
MID_BATCHES = (
    2, 3, 2, 1, 1, 3, 1, 5, 7, 6, 5, 5, 4, 3, 5, 2,
    7, 6, 7, 6, 5, 3, 1, 4, 4, 5, 7, 6, 5, 4, 0, 1,
    4, 7, 0, 0, 6, 6, 0, 2, 4, 7, 7, 3, 6, 3, 2, 2,
    5, 1, 0, 1, 3, 2, 3, 0, 7, 0, 0, 4, 4, 2, 6, 1,
)
END_ORDER = (
    500, 0, 400, 800, 900, 510, 501, 700, 1, 10, 410, 401, 100, 801, 710, 901,
    810, 701, 910, 520, 420, 11, 300, 101, 20, 511, 711, 811, 820, 411, 200, 911,
    530, 10000, 720, 10010, 301, 600, 10020, 21, 430, 10030, 521, 30, 821, 10040, 421, 10050,
    531, 201, 431, 721, 830, 20520, 601, 20411, 20511, 20711, 20020, 10100, 920, 10110, 31, 20810,
    20010, 610, 10120, 831, 10130, 930, 20011, 10140, 730, 10150, 921, 20710, 20811, 230, 611, 20530,
    130, 20021, 20721, 10200, 931, 331, 20821, 731, 10210, 20911, 10220, 630, 20820, 10230, 620, 131,
    20910, 10240, 10250, 110, 20720, 10300, 10310, 631, 20510, 20030, 20201, 20421, 231, 10320, 210, 20930,
    621, 20611, 10330, 10340, 120, 111, 20531, 20521, 10350, 310, 20431, 20410, 20401, 10400, 220, 20420,
    10410, 20131, 20031, 20921, 20331, 211, 10420, 10430, 121, 330, 20301, 20931, 10440, 10450, 311, 20430,
    20601, 10500, 320, 10510, 20130, 20830, 20731, 20231, 10520, 221, 20831, 10530, 20631, 20920, 321, 10540,
    20101, 10550, 10600, 20730, 10610, 10620, 20230, 20121, 20621, 20610, 10630, 10640, 20630, 10650, 20001, 10700,
    10710, 20330, 20221, 20120, 20321, 10720, 10730, 20620, 20111, 10740, 20100, 20000, 10750, 20211, 20220, 20311,
    20320, 20901, 20110, 20701, 20501, 20210, 20801, 20200, 20310, 20600, 20900, 20300, 20700, 20500, 20400, 20800,
)
MID_ORDER = (
    500, 0, 400, 800, 700, 900, 510, 530, 1, 30, 410, 10, 801, 430, 701, 501,
    810, 830, 901, 401, 520, 531, 31, 431, 710, 20, 730, 11, 930, 811, 420, 831,
    511, 130, 711, 411, 521, 330, 21, 421, 731, 820, 910, 931, 230, 10000, 600, 131,
    10010, 821, 920, 10020, 331, 10030, 720, 630, 911, 10040, 220, 10050, 601, 120, 10100, 921,
    231, 10110, 321, 721, 20731, 20510, 20411, 10120, 620, 10130, 631, 10140, 610, 121, 10150, 10200,
    100, 10210, 10220, 20331, 20701, 221, 621, 10230, 200, 611, 10240, 10250, 101, 110, 20011, 10300,
    300, 10310, 20010, 10320, 20131, 210, 10330, 20811, 20721, 201, 10340, 20711, 10350, 320, 20631, 111,
    20810, 10400, 20431, 301, 10410, 20001, 20020, 10420, 310, 10430, 20710, 20121, 10440, 20621, 20511, 211,
    10450, 10500, 311, 20221, 20410, 10510, 20030, 20021, 20231, 20000, 20920, 10520, 10530, 20611, 20911, 10540,
    10550, 20921, 20321, 10600, 20801, 10610, 20301, 20031, 20700, 20120, 10620, 20820, 10630, 20901, 20821, 10640,
    20111, 20910, 20931, 10650, 20800, 20720, 10700, 20130, 10710, 20101, 20421, 20520, 20521, 20220, 20930, 20830,
    20201, 10720, 20831, 10730, 20211, 10740, 20730, 20620, 10750, 20531, 20530, 20311, 20320, 20420, 20601, 20230,
    20900, 20110, 20501, 20401, 20630, 20610, 20330, 20210, 20430, 20310, 20500, 20100, 20400, 20600, 20200, 20300,
)
ORDERS = (END_ORDER, MID_ORDER)


def expert_ffn(rows, gate_weight, up_weight, down_weight):
    gate = jnp.dot(rows, gate_weight, preferred_element_type=jnp.float32)
    up_part = jnp.dot(rows, up_weight, preferred_element_type=jnp.float32)
    hidden = (jax.nn.silu(gate) * up_part).astype(jnp.bfloat16)
    return jnp.dot(hidden, down_weight, preferred_element_type=jnp.float32).astype(jnp.bfloat16)


def blockwise(rows, live_rows, weights):
    turns = (live_rows + 127) // 128

    def step(block_index, result):
        first_row = block_index * 128
        block_rows = lax.dynamic_slice_in_dim(rows, first_row, 128, 0)
        answer = expert_ffn(block_rows, weights[0], weights[1], weights[2])
        return lax.dynamic_update_slice_in_dim(result, answer, first_row, 0)

    return lax.fori_loop(jnp.int32(0), turns, step, jnp.zeros(rows.shape, jnp.bfloat16))


def per_device(tokens, expert_ids, route_logits, w_gate, w_up, w_down):
    tok_rows, model_width = tokens.shape
    picks = expert_ids.shape[1]
    experts = lax.axis_size("ep")
    capacity = min(tok_rows, 3 * tok_rows * picks // (2 * experts))
    row_quota = tok_rows * picks
    received = experts * capacity
    spill_count = (max(received - row_quota, 128) + 127) // 128 * 128
    length = row_quota + spill_count
    flat_ids = expert_ids.reshape(-1)
    one_hot = (flat_ids[:, None] == jnp.arange(experts, dtype=jnp.int32)[None, :]).astype(jnp.int32)
    earlier = jnp.cumsum(one_hot, axis=0) - one_hot
    slot_rank = jnp.sum(earlier * one_hot, axis=1)
    counts = jnp.sum(one_hot, axis=0)
    slot_place = flat_ids * capacity + slot_rank
    source_row = jnp.arange(row_quota, dtype=jnp.int32) // picks
    slot_token = jnp.full((received,), tok_rows, jnp.int32).at[slot_place].set(source_row)
    padded_tokens = jnp.concatenate([tokens, jnp.zeros((1, model_width), tokens.dtype)], 0)
    outgoing = padded_tokens[slot_token].reshape(experts, capacity, model_width)
    all_counts = lax.all_gather(counts, "ep", axis=0, tiled=True).reshape(experts, experts)
    own_index = lax.axis_index("ep")
    from_sources = lax.dynamic_index_in_dim(all_counts, own_index, 1, keepdims=False)
    incoming = lax.all_to_all(outgoing, "ep", split_axis=0, concat_axis=0, tiled=True)
    offsets = jnp.cumsum(from_sources) - from_sources
    live_rows = jnp.sum(from_sources)
    slot_numbers = jnp.arange(capacity, dtype=jnp.int32)
    live_slot = slot_numbers[None, :] < from_sources[:, None]
    position = jnp.where(live_slot, offsets[:, None] + slot_numbers[None, :], length).reshape(-1)
    gather_order = (
        jnp.full((length,), received, jnp.int32)
        .at[position]
        .set(jnp.arange(received, dtype=jnp.int32), mode="drop")
    )
    flat_incoming = jnp.concatenate(
        [incoming.reshape(received, model_width), jnp.zeros((1, model_width), jnp.bfloat16)], 0
    )
    packed = flat_incoming[gather_order]
    own_weights = (w_gate[0], w_up[0], w_down[0])
    results = blockwise(packed, live_rows, own_weights)
    results_ext = jnp.concatenate([results, jnp.zeros((1, model_width), jnp.bfloat16)], 0)
    outgoing_back = results_ext[position].reshape(experts, capacity, model_width)
    answers = lax.all_to_all(outgoing_back, "ep", split_axis=0, concat_axis=0, tiled=True)
    mix_weights = jax.nn.softmax(route_logits, axis=-1)
    picked = answers.reshape(received, model_width)[slot_place].reshape(
        tok_rows, picks, model_width
    )
    mixed_rows = jnp.zeros((tok_rows, model_width), jnp.float32)
    for column in range(picks):
        mixed_rows = mixed_rows + mix_weights[:, column : column + 1] * picked[:, column].astype(
            jnp.float32
        )
    return mixed_rows.astype(jnp.bfloat16)


def remote(src, dst, send_sem, recv_sem, target):
    return pltpu.make_async_remote_copy(
        src_ref=src,
        dst_ref=dst,
        send_sem=send_sem,
        recv_sem=recv_sem,
        device_id={"ep": target},
        device_id_type=pl.DeviceIdType.MESH,
    )


SENDS = len(GATHER_X)
PIECES = len(END_BATCHES) // 8
CELLS = [(h, d, c) for h in range(SENDS) for d in range(4) for c in range(2)]


def slots_of(batches):
    filled, table = [0] * PIECES, {}
    places = [(piece, d, c) for piece in range(PIECES) for d in range(4) for c in range(2)]
    for (piece, d, c), batch in zip(places, batches):
        for p in range(SENDS):
            if PARTS[p] == piece:
                table[p, d, c] = (batch, filled[batch])
        filled[batch] += 1
    return table


SLOT = (slots_of(END_BATCHES), slots_of(MID_BATCHES))


def at(cell):
    return (cell[0] * 4 + cell[1]) * 2 + cell[2]


def place_of(cell):
    return cell[1] * 2 + cell[2]


def moves(role, cell):
    p, d, c = cell
    first_z = not GATHER_X[p]
    out = []
    if d == 0 and (c == 0 or not first_z):
        if role == 0:
            out.append(("in", 1, (p, 3, c)))
        else:
            out.append(("out", 0, (p, 1, c)))
            out.append(("in", 1, (p, 1, c)))
    elif d > 0 and (c == 0 or not first_z) and role == 1:
        if d == 3:
            out.append(("in", 1, (p, 2, c)))
        else:
            out.append(("out", 0, (p, d + 1, c)))
    if c == 0 and (first_z or d == 0):
        across = ("x", role, (p, d, 1))
        out = out + [across] if first_z else [across] + out
    return out


def fused_kernel(
    n,
    tok_ref,
    ids_hbm,
    logits_hbm,
    wg_hbm,
    wu_hbm,
    wd_hbm,
    out_ref,
    xs,
    wg,
    wu,
    wd,
    ps,
    sib,
    put,
    got_x,
    got_in,
    got_out,
    hid,
    ids_ref,
    logits_ref,
    gates,
    gate_tok,
    gate_col,
    load_sem,
    tok_sem,
    ag_send,
    ag_recv,
    twin_send,
    twin_recv,
    gate_send,
    gate_recv,
    gate_pass,
    sib_send,
    sib_recv,
    rs_send,
    x_recv,
    in_recv,
    out_recv,
):
    tok_rows, width = tok_ref.shape
    rows = tok_rows // PIECES
    ff = wg.shape[1]
    ff_tile = ff // 4
    out_tile = width // 2
    me = lax.axis_index("ep")
    core, chip = me % 2, me // 2
    other = 1 - core
    x, z = chip % 2, chip // 2
    depth = n // 4
    inward = jnp.where(z < depth // 2, 1, -1)
    at_end = jnp.logical_or(z == 0, z == depth - 1)
    at_mid = jnp.logical_not(at_end)
    peers = {
        "in": ((z + inward) * 2 + x) * 2 + other,
        "out": ((z - inward) * 2 + x) * 2 + other,
        "x": (z * 2 + 1 - x) * 2 + other,
        "twin": chip * 2 + other,
    }

    def by_role(end_part, mid_part):
        if end_part is not None:
            pl.when(at_end)(end_part)
        if mid_part is not None:
            pl.when(at_mid)(mid_part)

    barrier = pltpu.get_barrier_semaphore()

    def greet(friend):
        pl.semaphore_signal(
            barrier,
            inc=1,
            device_id={"ep": peers[friend]},
            device_id_type=pl.DeviceIdType.MESH,
        )

    greet("twin")
    greet("x")
    greet("in")
    by_role(None, lambda: greet("out"))

    small_loads = [
        pltpu.make_async_copy(ids_hbm, ids_ref, load_sem.at[3]),
        pltpu.make_async_copy(logits_hbm, logits_ref, load_sem.at[4]),
    ]
    for load in small_loads:
        load.start()

    def cols_of(cell):
        piece = PARTS[cell[0]]
        part_width = width // PARTS.count(piece)
        return pl.ds((cell[0] - PARTS.index(piece)) * part_width, part_width)

    def chunk(role, cell, whose):
        batch, place = SLOT[role][cell]
        return xs.at[(batch * PIECES + place) * 2 + whose, :, cols_of(cell)]

    def own_load(role, p):
        return pltpu.make_async_copy(
            tok_ref.at[pl.ds(PARTS[p] * rows, rows), cols_of((p, 0, 0))],
            chunk(role, (p, 0, 0), core),
            tok_sem.at[p],
        )

    def load_all(role):
        for code in ORDERS[role]:
            if code // 10000 == 0 and code % 100 == 0:
                own_load(role, code // 100).start()

    by_role(lambda: load_all(0), lambda: load_all(1))
    weight_loads = [
        pltpu.make_async_copy(wg_hbm.at[0], wg, load_sem.at[0]),
        pltpu.make_async_copy(wu_hbm.at[0], wu, load_sem.at[1]),
        pltpu.make_async_copy(wd_hbm.at[0], wd, load_sem.at[2]),
    ]

    def own_gates():
        for load in small_loads:
            load.wait()
        logits = logits_ref[...]
        powers = jnp.exp(logits - jnp.max(logits, axis=0, keepdims=True))
        shares = powers / jnp.sum(powers, axis=0, keepdims=True)
        ids = ids_ref[...]
        for expert in range(n):
            gates[core, pl.ds(expert, 1), :] = jnp.sum(
                jnp.where(ids == expert, shares, 0.0), axis=0, keepdims=True
            )

    by_role(lambda: pl.semaphore_wait(barrier, 3), lambda: pl.semaphore_wait(barrier, 4))
    for load in weight_loads:
        load.start()

    def ag_copy(role, cell, link, to_role, to_cell):
        return remote(
            chunk(role, cell, core),
            chunk(to_role, to_cell, other),
            ag_send.at[0],
            ag_recv.at[at(to_cell)],
            peers[link],
        )

    def pass_copy(role, cell, whose):
        batch, place = SLOT[role][cell]
        ref = chunk(role, cell, whose)
        return remote(ref, ref, twin_send.at[0], twin_recv.at[batch], peers["twin"])

    def gate_copy(cell, link, to_cell):
        return remote(
            gates.at[place_of(cell) * 2 + core],
            gates.at[place_of(to_cell) * 2 + other],
            gate_send.at[0],
            gate_recv.at[place_of(to_cell)],
            peers[link],
        )

    def gate_twin(cell, whose):
        place = place_of(cell)
        ref = gates.at[place * 2 + whose]
        return remote(ref, ref, gate_send.at[1], gate_pass.at[place], peers["twin"])

    def receive(role, cell):
        p, d, c = cell
        lead = p == 0
        if (d, c) == (0, 0):
            if lead:
                own_gates()
            own_load(role, p).wait()
        else:
            if lead:
                gate_copy(cell, "x", cell).wait_recv()
            ag_copy(role, cell, "x", role, cell).wait_recv()
        for link, to_role, to_cell in moves(role, cell):
            if lead:
                gate_copy(cell, link, to_cell).start()
            ag_copy(role, cell, link, to_role, to_cell).start()
        if lead:
            gate_twin(cell, core).start()
        pass_copy(role, cell, core).start()

    def sib_copy(batch, part, whose):
        cols = pl.ds(pl.multiple_of(part * out_tile, out_tile), out_tile)
        return remote(
            ps.at[batch, :, whose, :, cols],
            sib.at[batch, :, :, cols],
            sib_send.at[0],
            sib_recv.at[batch],
            peers["twin"],
        )

    sib_seen = (set(), set())
    put_used = [0, 0]

    def send_back(role, cell):
        p, d, c = cell
        first_z = not SUM_Z[p]
        batch, place = SLOT[role][cell]
        cols = cols_of(cell)
        if batch not in sib_seen[role]:
            sib_seen[role].add(batch)
            ref = sib.at[batch]
            remote(ref, ref, sib_send.at[0], sib_recv.at[batch], peers["twin"]).wait_recv()
        total = ps[batch, place, core, :, cols].astype(jnp.float32)
        total = total + sib[batch, place, :, cols].astype(jnp.float32)
        inbox = []
        if c == 0 and (first_z or d == 0):
            inbox.append((got_x, x_recv, p * 4 + d))
        if c == 0 or not first_z:
            if d == 0 or (d == 3 and role == 1):
                inbox.append((got_in, in_recv, (p * 2 + d // 3) * 2 + c))
            if role == 1 and d < 3:
                inbox.append((got_out, out_recv, (p * 3 + d) * 2 + c))
        for buffer, sem, index in inbox:
            ref = buffer.at[index, :, pl.ds(0, cols.size)]
            remote(ref, ref, rs_send.at[0], sem.at[index], peers["x"]).wait_recv()
            total = total + buffer[index, :, pl.ds(0, cols.size)].astype(jnp.float32)
        total = total.astype(jnp.bfloat16)
        if c == 1 and (first_z or d == 0):
            link, buffer, sem, index = "x", got_x, x_recv, p * 4 + d
        elif d == 0:
            out_ref[pl.ds(PARTS[p] * rows, rows), cols] = total
            return
        elif role == 0:
            link, buffer, sem, index = "in", got_out, out_recv, (p * 3 + d - 1) * 2 + c
        elif d == 3:
            link, buffer, sem, index = "out", got_in, in_recv, p * 4 + c
        else:
            link, buffer, sem, index = "in", got_in, in_recv, (p * 2 + d - 1) * 2 + c
        slot = put_used[role]
        put_used[role] += 1
        used = pl.ds(0, cols.size)
        put[slot, :, used] = total
        remote(
            put.at[slot, :, used],
            buffer.at[index, :, used],
            rs_send.at[0],
            sem.at[index],
            peers[link],
        ).start()

    def hidden_part(batch, first, last):
        def body(j, carry):
            rows_in = xs[pl.ds(batch * 2 * PIECES, 2 * PIECES)].reshape(2 * tok_rows, width)
            cols = pl.ds(pl.multiple_of(j * ff_tile, ff_tile), ff_tile)
            gate = jnp.dot(rows_in, wg[:, cols], preferred_element_type=jnp.float32)
            up = jnp.dot(rows_in, wu[:, cols], preferred_element_type=jnp.float32)
            hid[:, cols] = (gate / (1.0 + jnp.exp(-gate)) * up).astype(jnp.bfloat16)
            return carry

        lax.fori_loop(first, last, body, 0)

    def answer_part(batch, first, last):
        def body(j, carry):
            cols = pl.ds(pl.multiple_of(j * out_tile, out_tile), out_tile)
            answer = jnp.dot(hid[...], wd[:, cols], preferred_element_type=jnp.float32)
            scale = jnp.concatenate([gate_col[...]] * (out_tile // 128), axis=1)
            ps[batch, :, :, :, cols] = (
                (answer * scale).astype(jnp.bfloat16).reshape(PIECES, 2, rows, out_tile)
            )
            sib_copy(batch, j, other).start()
            return carry

        lax.fori_loop(first, last, body, 0)

    gates_seen = (set(), set())

    def gate_fill(role, batch):
        for cell in CELLS:
            p, d, c = cell
            if SLOT[role][cell][0] != batch or PARTS.index(PARTS[p]) != p:
                continue
            source = place_of(cell)
            if source not in gates_seen[role]:
                gates_seen[role].add(source)
                gate_twin((0, d, c), other).wait_recv()
                for whose in range(2):
                    row = gates[source * 2 + whose, pl.ds(me, 1), :]
                    gate_tok[source * 2 + whose] = jnp.broadcast_to(row, (128, tok_rows)).T
            for whose in range(2):
                first = (SLOT[role][cell][1] * 2 + whose) * rows
                gate_col[pl.ds(first, rows), :] = gate_tok[
                    source * 2 + whose, pl.ds(PARTS[p] * rows, rows), :
                ]

    def compute(batch, first, last):
        if first == 0:
            ref = xs.at[pl.ds(0, PIECES)]
            remote(ref, ref, twin_send.at[0], twin_recv.at[batch], peers["twin"]).wait_recv()
            if batch == 0:
                weight_loads[0].wait()
                weight_loads[1].wait()
        if first < 4:
            hidden_part(batch, first, min(last, 4))
        if first <= 4 < last:
            by_role(lambda: gate_fill(0, batch), lambda: gate_fill(1, batch))
            if batch == 0:
                weight_loads[2].wait()
        if last > 4:
            answer_part(batch, max(first, 4) - 4, last - 4)

    def events(role, codes):
        if not codes:
            return None

        def run():
            for code in codes:
                cell = (code // 100 % 100, code // 10 % 10, code % 10)
                if code < 10000:
                    receive(role, cell)
                else:
                    send_back(role, cell)

        return run

    plans = []
    for order in ORDERS:
        plan, now = [], []
        for code in order:
            if code // 10000 == 1:
                plan.append((now, code))
                now = []
            else:
                now.append(code)
        plan.append((now, None))
        plans.append(plan)

    waiting = None
    for (end_codes, code), (mid_codes, mid_code) in zip(*plans):
        assert code == mid_code
        batch, part = (None, None) if code is None else (code // 100 % 100, code // 10 % 10)
        if waiting is not None and (end_codes or mid_codes or batch != waiting[0]):
            compute(*waiting)
            waiting = None
        by_role(events(0, end_codes), events(1, mid_codes))
        if code is not None:
            waiting = (batch, part, part + 1) if waiting is None else (batch, waiting[1], part + 1)

    def finish(role):
        sent = sum(len(moves(role, cell)) * 2 // PARTS.count(PARTS[cell[0]]) for cell in CELLS)
        ref = xs.at[pl.ds(0, sent // 2)]
        remote(ref, ref, ag_send.at[0], ag_recv.at[0], peers["x"]).wait_send()
        sent = sum(len(moves(role, cell)) for cell in CELLS if cell[0] == 0)
        ref = gates.at[pl.ds(0, sent)]
        remote(ref, ref, gate_send.at[0], gate_recv.at[0], peers["x"]).wait_send()

    by_role(lambda: finish(0), lambda: finish(1))
    ref = xs.at[pl.ds(0, len(END_BATCHES))]
    remote(ref, ref, twin_send.at[0], twin_recv.at[0], peers["twin"]).wait_send()
    ref = gates.at[pl.ds(0, 8)]
    remote(ref, ref, gate_send.at[1], gate_pass.at[0], peers["twin"]).wait_send()
    remote(sib, sib, sib_send.at[0], sib_recv.at[0], peers["twin"]).wait_send()
    assert put_used == [SENDS * 7] * 2
    ref = put.at[pl.ds(0, PIECES * 7)]
    remote(ref, ref, rs_send.at[0], x_recv.at[0], peers["x"]).wait_send()


def fused_scratch(n, tok_rows, width, ff, picks):
    bf16, f32 = jnp.bfloat16, jnp.float32
    rows = tok_rows // PIECES
    chunk = (rows, width)
    buffers = [
        ((PIECES * 16,) + chunk, bf16),
        ((width, ff), bf16),
        ((width, ff), bf16),
        ((ff, width), bf16),
        ((PIECES, 8, 2) + chunk, bf16),
        ((PIECES, 8) + chunk, bf16),
        ((SENDS * 7,) + chunk, bf16),
        ((SENDS * 4,) + chunk, bf16),
        ((SENDS * 4,) + chunk, bf16),
        ((SENDS * 6,) + chunk, bf16),
        ((2 * tok_rows, ff), bf16),
        ((picks, tok_rows), jnp.int32),
        ((picks, tok_rows), f32),
        ((16, n, tok_rows), f32),
        ((16, tok_rows, 128), f32),
        ((2 * tok_rows, 128), f32),
    ]
    sems = [5, SENDS, 1, SENDS * 8, 1, PIECES, 2, 8, 8, 1, PIECES, 1]
    sems += [SENDS * 4, SENDS * 4, SENDS * 6]
    size = 0
    for shape, kind in buffers:
        count = jnp.dtype(kind).itemsize
        for extent in shape:
            count = count * extent
        size = size + count
    scratch = [pltpu.VMEM(shape, kind) for shape, kind in buffers]
    return scratch + [pltpu.SemaphoreType.DMA((count,)) for count in sems], size


def fused_device(tokens, expert_ids, route_logits, w_gate, w_up, w_down):
    n = lax.axis_size("ep")
    tok_rows, width = tokens.shape
    ff = w_gate.shape[2]
    scratch, size = fused_scratch(n, tok_rows, width, ff, expert_ids.shape[1])
    anywhere, vmem = pl.BlockSpec(memory_space=pl.ANY), pl.BlockSpec(memory_space=pltpu.VMEM)
    return pl.pallas_call(
        functools.partial(fused_kernel, n),
        out_shape=pltpu.VMEM((tok_rows, width), jnp.bfloat16),
        in_specs=[anywhere] * 6,
        out_specs=vmem,
        scratch_shapes=scratch,
        compiler_params=pltpu.CompilerParams(
            collective_id=0, has_side_effects=True, vmem_limit_bytes=VMEM_BYTES
        ),
    )(tokens, expert_ids.T, route_logits.T, w_gate, w_up, w_down)


def layer(tokens, expert_ids, route_logits, w_gate, w_up, w_down):
    n = lax.axis_size("ep")
    tok_rows, width = tokens.shape
    ff = w_gate.shape[2]
    size = fused_scratch(n, tok_rows, width, ff, expert_ids.shape[1])[1]
    fits = size + 8 * tok_rows * width < VMEM_BYTES and width % 512 == 0 and ff % 512 == 0
    if fits and n == 16 and tok_rows == 16 * PIECES:
        return fused_device(tokens, expert_ids, route_logits, w_gate, w_up, w_down)
    return per_device(tokens, expert_ids, route_logits, w_gate, w_up, w_down)


def solution(mesh):
    in_specs = (
        P(("dp", "ep"), None),
        P(("dp", "ep"), None),
        P(("dp", "ep"), None),
        P("ep", None, None),
        P("ep", None, None),
        P("ep", None, None),
    )
    out_specs = P(("dp", "ep"), None)
    return jax.shard_map(
        layer, mesh=mesh, in_specs=in_specs, out_specs=out_specs, check_vma=False
    )
```
